512 devices in a mesh: image: 4 (over y), crop: 8 (over x, core), proto: 16 (over z).
Axes of the slice: x: 4, y: 4, z: 16, core: 2. Of those that a mesh axis runs over, the one named last changes fastest.
Arguments:
- teacher_feats: bfloat16 [256, 2, 512], P('image'), may hold values from -4 to 4
- student_feats: bfloat16 [8, 256, 512], P('crop', 'image'), may hold values from -4 to 4
- teacher_protos: bfloat16 [512, 262144], P(None, ('crop', 'proto')), may hold values from -6 to 6
- student_protos: bfloat16 [512, 262144], P(None, ('crop', 'proto')), may hold values from -6 to 6
- pairing: int32 [8, 256], P('crop', 'image'), may hold values from 0 to 1
- row_weight: bfloat16 [8, 256], P('crop', 'image'), may hold values from 0.5 to 4
Outputs:
- feat_grad: float32 [8, 256, 512], P('crop', 'image')
- row_loss: float32 [8, 256], P('crop', 'image')
The draws below stay inside these ranges and needn't reach their ends.
All inputs are finite; a program needn't handle non-finite values.
Results may differ from the reference program's by a relative error of at most 0.0016.
Values may be sent and summed in bfloat16 or wider, within the bound.
A program may use at most 64 MiB of HBM per device.

```python
import math
import jax
import jax.numpy as jnp
from jax import lax

D = 512
LOCAL = 8
GLOBAL = 2
SWEEPS = 3
IMAGES = 256
PROTOS = 262144


concept_count = 32


def concept_directions(key):
    return jax.random.normal(jax.random.fold_in(key, 7001), (concept_count, D), jnp.float32)


def image_concepts(key):
    return jax.random.randint(jax.random.fold_in(key, 7002), (IMAGES, 3), 0, concept_count)


def placed_protos(key):
    sub_key = jax.random.fold_in(key, 7003)
    entries = jax.random.normal(sub_key, (D, PROTOS), jnp.float32)
    directions = concept_directions(key)
    position = jnp.arange(PROTOS, dtype=jnp.float32) / PROTOS
    member_draw = jax.random.uniform(jax.random.fold_in(key, 7005), (PROTOS,), jnp.float32, 0.0, 1.0)
    member = member_draw < 0.25 + 0.5 * position
    owner = jax.random.randint(jax.random.fold_in(key, 7006), (PROTOS,), 0, concept_count)
    cosine = jax.random.uniform(jax.random.fold_in(key, 7007), (PROTOS,), jnp.float32, 0.3, 0.9)
    centre = directions[owner].T
    clustered = cosine[None, :] * centre + jnp.sqrt(1.0 - cosine * cosine)[None, :] * entries
    return jnp.where(member[None, :], clustered, entries)


def mixed_rows(key, salt, row_count):
    directions = concept_directions(key)[image_concepts(key)] / math.sqrt(D)
    mixture = jax.random.uniform(jax.random.fold_in(key, salt), (row_count, IMAGES, 3), jnp.float32, 0.0, 1.0)
    noise_term = 0.3 * jax.random.normal(jax.random.fold_in(key, salt + 1), (row_count, IMAGES, D), jnp.float32)
    return jnp.einsum('cij,ijd->cid', mixture, directions) + noise_term / math.sqrt(D)


def draw_teacher_feats(key, part):
    samples = 3.0 * mixed_rows(key, 7010, GLOBAL)
    return jnp.clip(jnp.transpose(samples, (1, 0, 2)), -4.0, 4.0).astype(jnp.bfloat16)


def draw_student_feats(key, part):
    samples = mixed_rows(key, 7020, LOCAL)
    lowest, highest = (0.05, 0.5)
    exponent = jax.random.uniform(jax.random.fold_in(key, 7030), (LOCAL, IMAGES, 1), jnp.float32, math.log(lowest), math.log(highest))
    return jnp.clip(samples * jnp.exp(exponent), -4.0, 4.0).astype(jnp.bfloat16)


def draw_student_protos(key, part):
    return jnp.clip(placed_protos(key), -6.0, 6.0).astype(jnp.bfloat16)


def draw_teacher_protos(key, part):
    drift_term = 0.3 * jax.random.normal(jax.random.fold_in(key, 7004), (D, PROTOS), jnp.float32)
    return jnp.clip(placed_protos(key) + drift_term, -6.0, 6.0).astype(jnp.bfloat16)


def set_ends(array, rng, least, high):
    dims = array.shape
    place = [jax.random.randint(jax.random.fold_in(rng, axis), (), 0, dims[axis]) for axis in range(len(dims))]
    array = array.at[tuple(place)].set(least)
    longest = dims.index(max(dims))
    place[longest] = (place[longest] + 1) % dims[longest]
    return array.at[tuple(place)].set(high)


def shard_levels(stream_key, shape, cuts, least, high):
    def one(axis_at, shards_of):
        heights = jax.random.uniform(jax.random.fold_in(jax.random.fold_in(stream_key, 6), axis_at), (shards_of,), jnp.float32, least / len(cuts), high / len(cuts))
        return jnp.repeat(jnp.exp(heights), shape[axis_at] // shards_of).reshape((-1,) + (1,) * (len(shape) - axis_at - 1))

    gain = one(*cuts[0])
    for cut in cuts[1:]:
        gain = gain * one(*cut)
    return gain


def setup_inputs(seed: int = 0) -> dict:
    seeds = jax.random.split(jax.random.key(seed), 7)
    return {
        "teacher_feats": draw_teacher_feats(jax.random.fold_in(seeds[6], 71), 0),
        "student_feats": draw_student_feats(jax.random.fold_in(seeds[6], 71), 0),
        "teacher_protos": draw_teacher_protos(jax.random.fold_in(seeds[6], 71), 0),
        "student_protos": draw_student_protos(jax.random.fold_in(seeds[6], 71), 0),
        "pairing": set_ends(jax.random.randint(seeds[4], (LOCAL, IMAGES), 0, GLOBAL), jax.random.fold_in(seeds[4], 1), 0, GLOBAL - 1).astype(jnp.int32),
        "row_weight": jnp.clip(jnp.exp(math.log(4.0) - 2.0794415 * jax.random.uniform(seeds[5], (LOCAL, IMAGES), jnp.float32) ** shard_levels(seeds[5], (LOCAL, IMAGES), ((0, 8), (1, 4)), -0.2, 0.2)), 0.5, 4.0).astype(jnp.bfloat16),
    }


epsilon = 1e-06
student_softness = 0.1
teacher_softness = 0.04

def unit_rows(raw_rows):
    return raw_rows * lax.rsqrt(lax.optimization_barrier(jnp.sum(raw_rows * raw_rows, axis=-1, keepdims=True)) + epsilon)

def unit_columns(weight_rows):
    entries = weight_rows.astype(jnp.float32)
    return (entries * lax.rsqrt(lax.optimization_barrier(jnp.sum(entries * entries, axis=0, keepdims=True)) + epsilon)).astype(jnp.bfloat16)

def finish_rows(raw_rows, back_sum, cross_term, running_sums):
    scales = lax.rsqrt(lax.optimization_barrier(jnp.sum(raw_rows * raw_rows, axis=-1, keepdims=True)) + epsilon)
    along = lax.optimization_barrier(jnp.sum(raw_rows * back_sum, axis=-1, keepdims=True))
    gradient = scales * back_sum - scales * scales * scales * raw_rows * along
    return (gradient, jnp.log(running_sums) - cross_term)

def reference(teacher_feats, student_feats, teacher_protos, student_protos, pairing, row_weight):
    teacher_normalized_rows = unit_rows(teacher_feats.astype(jnp.float32)).astype(jnp.bfloat16).reshape(IMAGES * GLOBAL, D)
    teacher_weight_matrix = unit_columns(teacher_protos)
    student_weight_matrix = unit_columns(student_protos)
    transport_plan = jnp.exp(jnp.dot(teacher_normalized_rows, teacher_weight_matrix, preferred_element_type=jnp.float32) / teacher_softness)
    for sweep_index in range(SWEEPS):
        transport_plan = transport_plan / lax.optimization_barrier(jnp.sum(transport_plan, axis=0, keepdims=True))
        transport_plan = transport_plan / lax.optimization_barrier(jnp.sum(transport_plan, axis=1, keepdims=True))
    targets = transport_plan.astype(jnp.bfloat16).reshape(IMAGES, GLOBAL, PROTOS)

    def crop_step(inputs):
        features, picked, weight_rows = inputs
        raw_rows = features.astype(jnp.float32)
        student_normalized_rows = unit_rows(raw_rows).astype(jnp.bfloat16)
        score_matrix = jnp.dot(student_normalized_rows, student_weight_matrix, preferred_element_type=jnp.float32) / student_softness
        exponent_terms = jnp.exp(score_matrix)
        running_sums = lax.optimization_barrier(jnp.sum(exponent_terms, axis=1))
        selected_entries = jnp.zeros(score_matrix.shape, jnp.float32)
        for view_index in range(GLOBAL):
            selected_entries = jnp.where((picked == view_index)[:, None], targets[:, view_index, :].astype(jnp.float32), selected_entries)
        cross_term = lax.optimization_barrier(jnp.sum(selected_entries * score_matrix, axis=1))
        linear_factors = (weight_rows.astype(jnp.float32)[:, None] * (exponent_terms / running_sums[:, None] - selected_entries) / student_softness).astype(jnp.bfloat16)
        back_sum = jnp.dot(linear_factors, student_weight_matrix.T, preferred_element_type=jnp.float32)
        return finish_rows(raw_rows, back_sum, cross_term, running_sums)
    gradients, losses = lax.map(crop_step, (student_feats, pairing, row_weight))
    return (gradients, losses)
```

```python
import functools

import jax
import jax.numpy as jnp
from jax import lax
from jax.experimental import pallas as pl
from jax.experimental.pallas import tpu as pltpu
from jax.sharding import PartitionSpec as P

EPSILON = 1e-06
MESH = pl.DeviceIdType.MESH
HIGHEST = lax.Precision.HIGHEST
F32 = jnp.float32
BF16 = jnp.bfloat16
NT = (((1,), (1,)), ((), ()))
ROWS = 512
COLS = 2048
LANES = 128
CHUNK = 256


def every(n, body):
    lax.fori_loop(0, n, lambda k, c: (body(k), c)[1], 0)


def unit_rows(x):
    return x * lax.rsqrt(jnp.sum(x * x, axis=1, keepdims=True) + EPSILON)


def unit_columns(raw, out):
    def chunk(j):
        cols = pl.ds(pl.multiple_of(j * LANES, LANES), LANES)
        w = raw[:, cols].astype(F32)
        scale = lax.rsqrt(jnp.sum(w * w, axis=0, keepdims=True) + EPSILON)
        out[:, cols] = (w * scale).astype(BF16)

    every(COLS // LANES, chunk)


def lane_sums(ref):
    ones = jnp.ones((8, LANES), F32)
    sums = lax.dot_general(ones, ref[...], NT, precision=HIGHEST, preferred_element_type=F32)
    return sums[0:1, :]


def kernel(
    y_n, c_n, z_n,
    tf_ref, sf_ref, pair_ref, weight_ref, tp_hbm, sp_hbm,
    grad_ref, loss_ref,
    tp, sp, wt, ws, t, e, tu, su, part, spart, ubuf, v, acc,
    r1p, r1z, r2p, r2z, a_out, a_in, az_out, az_in, a_all,
    ct_out, ct_in, cz_out, cz_in, c_tiles, ct_all, r3p, r3z,
    load, tu_s, tu_r, su_s, su_r, r1p_s, r1p_r, r1z_s, r1z_r, r2p_s, r2p_r, r2z_s, r2z_r,
    a_s, a_r, az_s, az_r, ag_s, ag_r, ct_s, ct_r, cz_s, cz_r, cg_s, cg_r, ca_s, ca_r,
    r3p_s, r3p_r, r3z_s, r3z_r,
):
    my_y, my_c, my_z = (lax.axis_index(a) for a in ("image", "crop", "proto"))

    def far_first(k):
        step = k + 1
        return z_n // 2 + (1 - 2 * lax.rem(step, 2)) * (step // 2)

    def push(src, dst, sends, recvs, axis, peer):
        pltpu.make_async_remote_copy(
            src_ref=src, dst_ref=dst, send_sem=sends, recv_sem=recvs,
            device_id={axis: peer}, device_id_type=MESH,
        ).start()

    def to_crops(src, dst, sends, recvs):
        def one(k):
            peer = lax.rem(my_c + k + 1, c_n)
            push(src(peer), dst, sends, recvs, "crop", peer)

        every(c_n - 1, one)

    def to_protos(src, dst, sends, recvs):
        def one(k):
            peer = lax.rem(my_z + far_first(k), z_n)
            push(src(peer), dst, sends, recvs, "proto", peer)

        every(z_n - 1, one)

    def await_bytes(ref, n, sem):
        some = ref.at[pl.ds(0, n)]
        pltpu.make_async_copy(some, some, sem).wait()

    loads = [
        pltpu.make_async_copy(tp_hbm, tp, load.at[0]),
        pltpu.make_async_copy(sp_hbm, sp, load.at[1]),
    ]
    for copy in loads:
        copy.start()

    barrier = pltpu.get_barrier_semaphore()

    def greet(axis, me, n):
        def one(k):
            pl.semaphore_signal(
                barrier, inc=1, device_id={axis: lax.rem(me + k + 1, n)}, device_id_type=MESH
            )

        every(n - 1, one)

    greet("proto", my_z, z_n)
    greet("crop", my_c, c_n)
    greet("image", my_y, y_n)

    tu[my_y] = unit_rows(tf_ref[...].astype(F32)).astype(BF16)
    su[my_c] = unit_rows(sf_ref[...].astype(F32)).astype(BF16)

    pl.semaphore_wait(barrier, y_n + c_n + z_n - 3)

    def give_rows(k):
        peer = lax.rem(my_y + k + 1, y_n)
        push(tu.at[my_y], tu.at[my_y], tu_s, tu_r, "image", peer)

    every(y_n - 1, give_rows)
    to_crops(lambda peer: su.at[my_c], su.at[my_c], su_s, su_r)

    loads[0].wait()
    unit_columns(tp, wt)
    await_bytes(tu, y_n - 1, tu_r)

    def transport(j):
        cols = pl.ds(pl.multiple_of(j * CHUNK, CHUNK), CHUNK)
        rows = tu[...].reshape(ROWS, ROWS)
        entries = jnp.exp(jnp.dot(rows, wt[:, cols], preferred_element_type=F32) * 25.0)
        t[:, cols] = entries
        v[:, cols] = jnp.broadcast_to(1.0 / jnp.sum(entries, axis=0, keepdims=True), (8, CHUNK))

    every(COLS // CHUNK, transport)

    def row_pass():
        def block(r, carry):
            rows = pl.ds(pl.multiple_of(r * 8, 8), 8)
            total = t[rows, 0:LANES] * v[:, 0:LANES]
            for k in range(1, COLS // LANES):
                cols = slice(k * LANES, (k + 1) * LANES)
                total = total + t[rows, cols] * v[:, cols]
            part[rows, :] = total
            return carry

        lax.fori_loop(0, ROWS // 8, block, 0, unroll=4)
        return lane_sums(part)

    def column_pass(row_sums):
        u = 1.0 / row_sums
        for q in range(ROWS // LANES):
            piece = u[:, q * LANES : (q + 1) * LANES]
            ubuf[q * LANES : (q + 1) * LANES, :] = jnp.broadcast_to(piece, (LANES, LANES)).T

        def block(r, sums):
            rows = pl.ds(pl.multiple_of(r * 8, 8), 8)
            scale = ubuf[rows, :]
            return tuple(
                s + t[rows, k * LANES : (k + 1) * LANES] * scale for k, s in enumerate(sums)
            )

        zero = tuple(jnp.zeros((8, LANES), F32) for _ in range(COLS // LANES))
        sums = lax.fori_loop(0, ROWS // 8, block, zero, unroll=4)
        for k, s in enumerate(sums):
            v[:, k * LANES : (k + 1) * LANES] = jnp.broadcast_to(
                1.0 / jnp.sum(s, axis=0, keepdims=True), (8, LANES)
            )

    r1p[my_c] = row_pass()
    to_crops(lambda peer: r1p.at[my_c], r1p.at[my_c], r1p_s, r1p_r)

    loads[1].wait()
    unit_columns(sp, ws)

    await_bytes(r1p, c_n - 1, r1p_r)
    r1z[my_z] = jnp.sum(r1p[...], axis=0)
    to_protos(lambda peer: r1z.at[my_z], r1z.at[my_z], r1z_s, r1z_r)

    await_bytes(su, c_n - 1, su_r)
    spart[...] = jnp.zeros_like(spart)

    def student(j):
        cols = pl.ds(pl.multiple_of(j * CHUNK, CHUNK), CHUNK)
        rows = su[...].reshape(ROWS, ROWS)
        terms = jnp.exp(jnp.dot(rows, ws[:, cols], preferred_element_type=F32) * 10.0)
        spart[...] += terms[:, :LANES] + terms[:, LANES:]
        e[:, cols] = terms.astype(BF16)

    every(COLS // CHUNK, student)

    def student_back(j):
        some = pl.ds(pl.multiple_of(j * CHUNK, CHUNK), CHUNK)
        acc[...] = lax.dot_general(e[...], ws[some, :], NT, preferred_element_type=F32)
        a_out[:, :, some] = acc[...].astype(BF16).reshape(c_n, ROWS // c_n, CHUNK)

    every(ROWS // CHUNK, student_back)
    to_crops(lambda peer: a_out.at[peer], a_in.at[my_c], a_s, a_r)
    partial_totals = lane_sums(spart)

    await_bytes(r1z, z_n - 1, r1z_r)
    column_pass(jnp.sum(r1z[...], axis=0))
    r2p[my_c] = jnp.concatenate([row_pass(), partial_totals], axis=1)
    to_crops(lambda peer: r2p.at[my_c], r2p.at[my_c], r2p_s, r2p_r)
    await_bytes(r2p, c_n - 1, r2p_r)
    r2z[my_z] = jnp.sum(r2p[...], axis=0)
    to_protos(lambda peer: r2z.at[my_z], r2z.at[my_z], r2z_s, r2z_r)

    await_bytes(a_in, c_n - 1, a_r)
    a_in[my_c] = a_out[my_c]
    for g in range(8):
        rows = slice(g * 8, g * 8 + 8)
        total = a_in[0, rows, :].astype(F32)
        for k in range(1, c_n):
            total = total + a_in[k, rows, :].astype(F32)
        for h in range(2):
            az_out[2 * g + h] = total[:, h * 256 : (h + 1) * 256].astype(BF16)
    to_protos(lambda peer: az_out.at[peer], az_in.at[my_z], az_s, az_r)

    await_bytes(r2z, z_n - 1, r2z_r)
    second = jnp.sum(r2z[...], axis=0)
    totals = second[:, ROWS:]
    column_pass(second[:, :ROWS])

    own_rows = pl.ds(pl.multiple_of(my_y * LANES, LANES), LANES)
    for k in range(COLS // CHUNK):
        cols = slice(k * CHUNK, (k + 1) * CHUNK)
        scaled = t[own_rows, cols] * v[0:1, cols]
        e[0:LANES, cols] = scaled.astype(BF16)
        halves = scaled[:, :LANES] + scaled[:, LANES:]
        part[0:LANES, :] = halves if k == 0 else part[0:LANES, :] + halves
    r3p[my_c] = lane_sums(part.at[0:LANES])
    sums = lax.dot_general(e[0:LANES, :], ws[...], NT, preferred_element_type=F32)
    ct_out[...] = sums.astype(BF16).reshape(c_n, 16, ROWS)
    to_crops(lambda peer: ct_out.at[peer], ct_in.at[my_c], ct_s, ct_r)
    to_crops(lambda peer: r3p.at[my_c], r3p.at[my_c], r3p_s, r3p_r)
    ct_in[my_c] = ct_out[my_c]
    await_bytes(ct_in, c_n - 1, ct_r)
    await_bytes(r3p, c_n - 1, r3p_r)
    total = jnp.sum(ct_in[...].astype(F32), axis=0)
    for g in range(2):
        for k in range(4):
            tile = total[g * 8 : g * 8 + 8, k * LANES : (k + 1) * LANES]
            cz_out[4 * g + k] = tile.astype(BF16)
    r3z[my_z] = jnp.sum(r3p[...], axis=0)
    to_protos(lambda peer: cz_out.at[lax.rem(peer, 8)], cz_in.at[my_z], cz_s, cz_r)
    to_protos(lambda peer: r3z.at[my_z], r3z.at[my_z], r3z_s, r3z_r)
    cz_in[my_z] = cz_out[lax.rem(my_z, 8)]

    await_bytes(az_in, z_n - 1, az_r)
    az_in[my_z] = az_out[my_z]
    a_all[my_z] = jnp.sum(az_in[...].astype(F32), axis=0)
    to_protos(lambda peer: a_all.at[my_z], a_all.at[my_z], ag_s, ag_r)

    await_bytes(cz_in, z_n - 1, cz_r)
    mine = lax.rem(my_z, 8)
    c_tiles[mine] = jnp.sum(cz_in[...].astype(F32), axis=0)

    def near(k):
        offset = k + z_n - 4 + jnp.where(k >= 4, 1, 0)
        peer = lax.rem(my_z + offset, z_n)
        push(c_tiles.at[mine], c_tiles.at[mine], cg_s, cg_r, "proto", peer)

    every(7, near)
    await_bytes(c_tiles, 7, cg_r)
    ct_all[my_c] = c_tiles[...]
    to_crops(lambda peer: c_tiles, ct_all.at[my_c], ca_s, ca_r)

    await_bytes(r3z, z_n - 1, r3z_r)
    last = 1.0 / jnp.sum(r3z[...], axis=0)
    await_bytes(a_all, z_n - 1, ag_r)

    images = ROWS // c_n
    lane = lax.broadcasted_iota(jnp.int32, (images, ROWS), 1)
    row = lax.broadcasted_iota(jnp.int32, (images, ROWS), 0)

    def as_column(values, first):
        wide = jnp.broadcast_to(values, (images, values.shape[1]))
        n = values.shape[1]
        picked = jnp.where(lane[:, :n] == row[:, :n] + first, wide, jnp.zeros_like(wide))
        return jnp.sum(picked, axis=1, keepdims=True)

    view = as_column(pair_ref[...].astype(F32), 0) > 0.5
    weight = as_column(weight_ref[...].astype(F32), 0)
    total_column = as_column(totals, my_c * images)
    scale_0 = as_column(last, 0)
    scale_1 = as_column(last, images)
    x = sf_ref[...].astype(F32)
    unit = su[my_c].astype(F32)
    norm = lax.rsqrt(jnp.sum(x * x, axis=1, keepdims=True) + EPSILON)
    log_total = jnp.log(total_column)
    first = jnp.concatenate(
        [jnp.concatenate([a_all[2 * g], a_all[2 * g + 1]], axis=1) for g in range(8)], axis=0
    ) / total_column

    await_bytes(ct_all, c_n - 1, ca_r)

    def summed(view_index):
        blocks = []
        for g in range(8):
            c, h = 4 * view_index + g // 2, g % 2
            blocks.append(jnp.concatenate([ct_all[c, 4 * h + k] for k in range(4)], axis=1))
        return jnp.concatenate(blocks, axis=0)

    chosen = jnp.where(view, summed(1) * scale_1, summed(0) * scale_0)
    back = (weight * 10.0) * (first - chosen)
    cross = jnp.sum(unit * chosen, axis=1, keepdims=True) * 10.0
    along = jnp.sum(x * back, axis=1, keepdims=True)
    grad_ref[...] = norm * back - norm * norm * norm * x * along
    losses = jnp.broadcast_to(log_total - cross, (images, images))
    eye = lane[:, :images] == row[:, :images]
    loss_ref[...] = jnp.sum(jnp.where(eye, losses, 0.0), axis=0, keepdims=True)

    for ref, n, sem in (
        (tu, y_n - 1, tu_s), (su, c_n - 1, su_s), (r1p, c_n - 1, r1p_s), (r1z, z_n - 1, r1z_s),
        (r2p, c_n - 1, r2p_s), (r2z, z_n - 1, r2z_s), (a_in, c_n - 1, a_s),
        (az_in, z_n - 1, az_s), (a_all, z_n - 1, ag_s), (ct_in, c_n - 1, ct_s),
        (cz_in, z_n - 1, cz_s), (c_tiles, 7, cg_s), (ct_all, c_n - 1, ca_s),
        (r3p, c_n - 1, r3p_s), (r3z, z_n - 1, r3z_s),
    ):
        await_bytes(ref, n, sem)


def solution(mesh):
    y_n, c_n, z_n = (mesh.shape[a] for a in ("image", "crop", "proto"))

    def step(teacher_feats, student_feats, teacher_protos, student_protos, pairing, row_weight):
        images, views, width = teacher_feats.shape
        teacher = jnp.transpose(teacher_feats, (1, 0, 2)).reshape(views * images, width)
        vmem = pl.BlockSpec(memory_space=pltpu.VMEM)
        hbm = pl.BlockSpec(memory_space=pl.ANY)
        dma = pltpu.SemaphoreType.DMA
        grad, loss = pl.pallas_call(
            functools.partial(kernel, y_n, c_n, z_n),
            out_shape=(
                jax.ShapeDtypeStruct((images, width), F32),
                jax.ShapeDtypeStruct((1, images), F32),
            ),
            in_specs=[vmem] * 4 + [hbm] * 2,
            out_specs=(vmem, vmem),
            scratch_shapes=[
                pltpu.VMEM((width, COLS), BF16),
                pltpu.VMEM((width, COLS), BF16),
                pltpu.VMEM((width, COLS), BF16),
                pltpu.VMEM((width, COLS), BF16),
                pltpu.VMEM((ROWS, COLS), F32),
                pltpu.VMEM((ROWS, COLS), BF16),
                pltpu.VMEM((y_n, views * images, width), BF16),
                pltpu.VMEM((c_n, images, width), BF16),
                pltpu.VMEM((ROWS, LANES), F32),
                pltpu.VMEM((ROWS, LANES), F32),
                pltpu.VMEM((ROWS, LANES), F32),
                pltpu.VMEM((8, COLS), F32),
                pltpu.VMEM((ROWS, CHUNK), F32),
                pltpu.VMEM((c_n, 1, ROWS), F32),
                pltpu.VMEM((z_n, 1, ROWS), F32),
                pltpu.VMEM((c_n, 1, 2 * ROWS), F32),
                pltpu.VMEM((z_n, 1, 2 * ROWS), F32),
                pltpu.VMEM((c_n, images, width), BF16),
                pltpu.VMEM((c_n, images, width), BF16),
                pltpu.VMEM((z_n, 8, 256), BF16),
                pltpu.VMEM((z_n, 8, 256), BF16),
                pltpu.VMEM((z_n, 8, 256), F32),
                pltpu.VMEM((c_n, 16, width), BF16),
                pltpu.VMEM((c_n, 16, width), BF16),
                pltpu.VMEM((8, 8, LANES), BF16),
                pltpu.VMEM((z_n, 8, LANES), BF16),
                pltpu.VMEM((8, 8, LANES), F32),
                pltpu.VMEM((c_n, 8, 8, LANES), F32),
                pltpu.VMEM((c_n, 1, LANES), F32),
                pltpu.VMEM((z_n, 1, LANES), F32),
                dma((2,)),
            ]
            + [dma(())] * 30,
            compiler_params=pltpu.CompilerParams(collective_id=0, has_side_effects=True),
        )(
            teacher,
            student_feats.reshape(images, width),
            pairing,
            row_weight,
            teacher_protos,
            student_protos,
        )
        return grad.reshape(1, images, width), loss

    return jax.shard_map(
        step,
        mesh=mesh,
        in_specs=(
            P("image", None, None),
            P("crop", "image", None),
            P(None, ("crop", "proto")),
            P(None, ("crop", "proto")),
            P("crop", "image"),
            P("crop", "image"),
        ),
        out_specs=(P("crop", "image", None), P("crop", "image")),
        check_vma=False,
    )
```

```python
import functools

import jax
import jax.numpy as jnp
from jax import lax
from jax.experimental import pallas as pl
from jax.experimental.pallas import tpu as pltpu
from jax.sharding import PartitionSpec as P

EPSILON = 1e-06
MESH = pl.DeviceIdType.MESH
F32 = jnp.float32
BF16 = jnp.bfloat16
NT = (((1,), (1,)), ((), ()))
ROWS = 512
COLS = 2048
LANES = 128
CHUNK = 256


def every(n, body):
    lax.fori_loop(0, n, lambda k, c: (body(k), c)[1], 0)


def unit_rows(x):
    return x * lax.rsqrt(jnp.sum(x * x, axis=1, keepdims=True) + EPSILON)


def unit_columns(raw, out):
    def chunk(j):
        cols = pl.ds(pl.multiple_of(j * LANES, LANES), LANES)
        w = raw[:, cols].astype(F32)
        scale = lax.rsqrt(jnp.sum(w * w, axis=0, keepdims=True) + EPSILON)
        out[:, cols] = (w * scale).astype(BF16)

    every(COLS // LANES, chunk)


def lane_sums(ref, groups):
    sums = [
        jnp.sum(ref[q * LANES : (q + 1) * LANES, :].T, axis=0, keepdims=True) for q in range(groups)
    ]
    return jnp.concatenate(sums, axis=0) if groups > 1 else sums[0]


def kernel(
    y_n, c_n, z_n,
    tf_hbm, sf_hbm, pair_hbm, weight_hbm, tp_hbm, sp_hbm,
    grad_ref, loss_ref,
    tf, sf, pair, weight, tp, sp, wt, ws, t, e, tu, su, part, spart, ubuf, v, csum,
    r1p, r1z, r2p, r2z, tot_p, tot_sum, tot_z, pairs,
    a_out, a_in, az_out, az_in, a_all,
    ct_out, ct_in, cz_out, cz_in, c_tiles, pick_out, pick_in, r3p, r3z,
    load, tu_r, th_r,
    tu_s, th_s, su_s, su_r, sh_s, sh_r, pr_s, pr_r, r1p_s, r1p_r, r1z_s, r1z_r,
    r2p_s, r2p_r, r2z_s, r2z_r, tp_s, tp_r, tz_s, tz_r, a_s, a_r, az_s, az_r, ag_s, ag_r,
    ct_s, ct_r, cz_s, cz_r, cg_s, cg_r, ca_s, ca_r, r3p_s, r3p_r, r3z_s, r3z_r,
):
    my_y, my_c, my_z = (lax.axis_index(a) for a in ("image", "crop", "proto"))
    side = lax.rem(my_c, 2)
    partner = my_c + 1 - 2 * side

    loads = [
        pltpu.make_async_copy(src, dst, load.at[k])
        for k, (src, dst) in enumerate(
            ((tf_hbm, tf), (sf_hbm, sf), (tp_hbm, tp), (sp_hbm, sp), (pair_hbm, pair), (weight_hbm, weight))
        )
    ]
    for copy in loads:
        copy.start()

    def far_first(k):
        step = k + 1
        return z_n // 2 + (1 - 2 * lax.rem(step, 2)) * (step // 2)

    def push(src, dst, sends, recvs, axis, peer):
        pltpu.make_async_remote_copy(
            src_ref=src, dst_ref=dst, send_sem=sends, recv_sem=recvs,
            device_id={axis: peer}, device_id_type=MESH,
        ).start()

    def to_crops(src, dst, sends, recvs):
        def one(k):
            peer = lax.rem(my_c + k + 1, c_n)
            push(src(peer), dst, sends, recvs, "crop", peer)

        every(c_n - 1, one)

    def to_protos(src, dst, sends, recvs):
        def one(k):
            peer = lax.rem(my_z + far_first(k), z_n)
            push(src(peer), dst, sends, recvs, "proto", peer)

        every(z_n - 1, one)

    def await_bytes(ref, n, sem):
        some = ref.at[pl.ds(0, n)]
        pltpu.make_async_copy(some, some, sem).wait()

    barrier = pltpu.get_barrier_semaphore()

    def greet(axis, me, n):
        def one(k):
            pl.semaphore_signal(
                barrier, inc=1, device_id={axis: lax.rem(me + k + 1, n)}, device_id_type=MESH
            )

        every(n - 1, one)

    greet("proto", my_z, z_n)
    greet("image", my_y, y_n)
    greet("crop", my_c, c_n)

    loads[0].wait()
    for g in range(2):
        tu[my_y, g] = unit_rows(tf[:, g, :].astype(F32)).astype(BF16)
    loads[1].wait()
    su[my_c] = unit_rows(sf[...].astype(F32)).astype(BF16)
    loads[4].wait()
    pairs[my_c] = pair[...].astype(F32)
    loads[2].wait()
    unit_columns(tp, wt)

    pl.semaphore_wait(barrier, y_n + c_n + z_n - 3)

    def give_rows(k):
        peer = lax.rem(my_y + 2 * k + 1 - 3 * (k // 2), y_n)
        push(tu.at[my_y, side], tu.at[my_y, side], tu_s, tu_r.at[my_y], "image", peer)

    every(y_n - 1, give_rows)

    def give_students(k):
        peer = lax.rem(my_c + 2 * k + 2, c_n)
        push(su.at[my_c], su.at[my_c], su_s, su_r, "crop", peer)

    every(c_n // 2 - 1, give_students)
    push(su.at[my_c], su.at[my_c], sh_s, sh_r, "crop", partner)
    to_crops(lambda peer: pairs.at[my_c], pairs.at[my_c], pr_s, pr_r)

    def transport(y, first):
        def chunk(j):
            cols = pl.ds(pl.multiple_of(j * CHUNK, CHUNK), CHUNK)
            rows = tu[y].reshape(LANES, ROWS)
            terms = jnp.exp(jnp.dot(rows, wt[:, cols], preferred_element_type=F32) * 25.0)
            t[pl.ds(pl.multiple_of(y * LANES, LANES), LANES), cols] = terms
            sums = jnp.sum(terms.reshape(LANES // 8, 8, CHUNK), axis=0)
            csum[:, cols] = sums if first else csum[:, cols] + sums

        every(COLS // CHUNK, chunk)

    def hand_over(y):
        pltpu.make_async_copy(tu.at[y, side], tu.at[y, side], tu_r.at[y]).wait()
        push(tu.at[y, side], tu.at[y, side], th_s, th_r.at[y], "crop", partner)

    def handed(y):
        pltpu.make_async_copy(tu.at[y, side], tu.at[y, side], th_r.at[y]).wait()

    others = [lax.rem(my_y + k, y_n) for k in (1, 3, 2)]
    transport(my_y, True)
    loads[3].wait()
    unit_columns(sp, ws)
    hand_over(others[0])
    hand_over(others[1])
    handed(others[0])
    transport(others[0], False)
    hand_over(others[2])
    handed(others[1])
    transport(others[1], False)
    handed(others[2])
    transport(others[2], False)

    def set_v(sums):
        for k, s in enumerate(sums):
            v[:, k * LANES : (k + 1) * LANES] = jnp.broadcast_to(
                1.0 / jnp.sum(s, axis=0, keepdims=True), (8, LANES)
            )

    set_v([csum[:, k * LANES : (k + 1) * LANES] for k in range(COLS // LANES)])

    def row_pass():
        def block(r, carry):
            rows = pl.ds(pl.multiple_of(r * 8, 8), 8)
            total = t[rows, 0:LANES] * v[:, 0:LANES]
            for k in range(1, COLS // LANES):
                cols = slice(k * LANES, (k + 1) * LANES)
                total = total + t[rows, cols] * v[:, cols]
            part[rows, :] = total
            return carry

        lax.fori_loop(0, ROWS // 8, block, 0, unroll=4)
        return lane_sums(part, 4)

    def column_pass(row_sums):
        u = 1.0 / row_sums
        for q in range(ROWS // LANES):
            ubuf[q * LANES : (q + 1) * LANES, :] = jnp.broadcast_to(u[q : q + 1, :], (LANES, LANES)).T

        def block(r, sums):
            rows = pl.ds(pl.multiple_of(r * 8, 8), 8)
            scale = ubuf[rows, :]
            return tuple(
                s + t[rows, k * LANES : (k + 1) * LANES] * scale for k, s in enumerate(sums)
            )

        zero = tuple(jnp.zeros((8, LANES), F32) for _ in range(COLS // LANES))
        set_v(lax.fori_loop(0, ROWS // 8, block, zero, unroll=4))

    r1p[my_c] = row_pass()
    to_crops(lambda peer: r1p.at[my_c], r1p.at[my_c], r1p_s, r1p_r)

    await_bytes(su, c_n // 2 - 1, su_r)

    def hand_students(k):
        slot = lax.rem(my_c + 2 * k + 2, c_n)
        push(su.at[slot], su.at[slot], sh_s, sh_r, "crop", partner)

    every(c_n // 2 - 1, hand_students)
    await_bytes(su, c_n // 2, sh_r)
    spart[...] = jnp.zeros_like(spart)

    def student(j):
        cols = pl.ds(pl.multiple_of(j * CHUNK, CHUNK), CHUNK)
        rows = su[...].reshape(ROWS, ROWS)
        terms = jnp.exp(jnp.dot(rows, ws[:, cols], preferred_element_type=F32) * 10.0)
        spart[...] += terms[:, :LANES] + terms[:, LANES:]
        e[:, cols] = terms.astype(BF16)

    every(COLS // CHUNK, student)

    await_bytes(r1p, c_n - 1, r1p_r)
    r1z[my_z] = jnp.sum(r1p[...], axis=0).astype(BF16)
    to_protos(lambda peer: r1z.at[my_z], r1z.at[my_z], r1z_s, r1z_r)

    for j in range(2):
        some = slice(j * CHUNK, (j + 1) * CHUNK)
        back = lax.dot_general(e[...], ws[some, :], NT, preferred_element_type=F32)
        a_out[:, :, some] = back.astype(BF16).reshape(c_n, ROWS // c_n, CHUNK)
    to_crops(lambda peer: a_out.at[peer], a_in.at[my_c], a_s, a_r)
    tot_p[my_c] = lane_sums(spart, 4)
    to_crops(lambda peer: tot_p.at[my_c], tot_p.at[my_c], tp_s, tp_r)

    await_bytes(r1z, z_n - 1, r1z_r)
    column_pass(jnp.sum(r1z[...].astype(F32), axis=0))
    r2p[my_c] = row_pass()
    to_crops(lambda peer: r2p.at[my_c], r2p.at[my_c], r2p_s, r2p_r)

    await_bytes(a_in, c_n - 1, a_r)
    a_in[my_c] = a_out[my_c]
    for g in range(8):
        rows = slice(g * 8, g * 8 + 8)
        total = a_in[0, rows, :].astype(F32)
        for k in range(1, c_n):
            total = total + a_in[k, rows, :].astype(F32)
        for h in range(2):
            az_out[2 * g + h] = total[:, h * 256 : (h + 1) * 256].astype(BF16)
    await_bytes(tot_p, c_n - 1, tp_r)
    whole = jnp.sum(tot_p[...], axis=0)
    for q in range(4):
        tot_sum[q] = whole[q : q + 1, :]
    tot_z[my_z] = tot_sum[my_c // 2]

    await_bytes(r2p, c_n - 1, r2p_r)
    r2z[my_z] = jnp.sum(r2p[...], axis=0).astype(BF16)
    to_protos(lambda peer: r2z.at[my_z], r2z.at[my_z], r2z_s, r2z_r)
    to_protos(lambda peer: az_out.at[peer], az_in.at[my_z], az_s, az_r)
    to_protos(lambda peer: tot_z.at[my_z], tot_z.at[my_z], tz_s, tz_r)

    await_bytes(r2z, z_n - 1, r2z_r)
    column_pass(jnp.sum(r2z[...].astype(F32), axis=0))

    own_rows = pl.ds(pl.multiple_of(my_y * LANES, LANES), LANES)
    for k in range(COLS // CHUNK):
        cols = slice(k * CHUNK, (k + 1) * CHUNK)
        scaled = t[own_rows, cols] * v[0:1, cols]
        e[0:LANES, cols] = scaled.astype(BF16)
        halves = scaled[:, :LANES] + scaled[:, LANES:]
        part[0:LANES, :] = halves if k == 0 else part[0:LANES, :] + halves
    r3p[my_c] = lane_sums(part, 1)
    to_crops(lambda peer: r3p.at[my_c], r3p.at[my_c], r3p_s, r3p_r)
    sums = lax.dot_general(e[0:LANES, :], ws[...], NT, preferred_element_type=F32)
    for c in range(c_n):
        for g in range(2):
            ct_out[c, g] = sums[64 * g + 8 * c : 64 * g + 8 * c + 8, :].astype(BF16)
    to_crops(lambda peer: ct_out.at[peer], ct_in.at[my_c], ct_s, ct_r)
    ct_in[my_c] = ct_out[my_c]

    await_bytes(az_in, z_n - 1, az_r)
    az_in[my_z] = az_out[my_z]
    a_all[my_z] = jnp.sum(az_in[...].astype(F32), axis=0)
    to_protos(lambda peer: a_all.at[my_z], a_all.at[my_z], ag_s, ag_r)

    await_bytes(r3p, c_n - 1, r3p_r)
    r3z[my_z] = jnp.sum(r3p[...], axis=0)
    to_protos(lambda peer: r3z.at[my_z], r3z.at[my_z], r3z_s, r3z_r)
    await_bytes(ct_in, c_n - 1, ct_r)
    total = jnp.sum(ct_in[...].astype(F32), axis=0)
    for g in range(2):
        for k in range(4):
            cz_out[4 * g + k] = total[g, :, k * LANES : (k + 1) * LANES].astype(BF16)
    to_protos(lambda peer: cz_out.at[lax.rem(peer, 8)], cz_in.at[my_z], cz_s, cz_r)
    cz_in[my_z] = cz_out[lax.rem(my_z, 8)]

    images = ROWS // c_n
    lane = lax.broadcasted_iota(jnp.int32, (images, LANES), 1)
    row = lax.broadcasted_iota(jnp.int32, (images, LANES), 0)

    def as_column(values, first, rows):
        n = values.shape[1]
        wide = jnp.broadcast_to(values, (rows, n))
        picked = jnp.where(lane[:rows, :n] == row[:rows, :n] + first, wide, jnp.zeros_like(wide))
        return jnp.sum(picked, axis=1, keepdims=True)

    loads[5].wait()
    weights = as_column(weight[...].astype(F32), 0, images)
    x = sf[...].astype(F32)
    unit = su[my_c].astype(F32)
    norm = lax.rsqrt(jnp.sum(x * x, axis=1, keepdims=True) + EPSILON)
    await_bytes(pairs, c_n - 1, pr_r)
    views = [as_column(pairs[c], my_c * 8, 8) > 0.5 for c in range(c_n)]
    await_bytes(tot_z, z_n - 1, tz_r)
    totals = as_column(jnp.sum(tot_z[...], axis=0), side * images, images)
    await_bytes(r3z, z_n - 1, r3z_r)
    last = 1.0 / jnp.sum(r3z[...], axis=0)
    scales = [as_column(last, images * g + my_c * 8, 8) for g in range(2)]

    await_bytes(cz_in, z_n - 1, cz_r)
    mine = lax.rem(my_z, 8)
    c_tiles[mine] = jnp.sum(cz_in[...].astype(F32), axis=0)

    def near(k):
        offset = k + z_n - 4 + jnp.where(k >= 4, 1, 0)
        peer = lax.rem(my_z + offset, z_n)
        push(c_tiles.at[mine], c_tiles.at[mine], cg_s, cg_r, "proto", peer)

    every(7, near)
    await_bytes(a_all, z_n - 1, ag_r)
    for g in range(8):
        for h in range(2):
            grad_ref[g * 8 : g * 8 + 8, h * 256 : (h + 1) * 256] = a_all[2 * g + h] / totals[g * 8 : g * 8 + 8]

    await_bytes(c_tiles, 7, cg_r)
    sides = [
        jnp.concatenate([c_tiles[4 * g + k] for k in range(4)], axis=1) * scales[g] for g in range(2)
    ]
    for c in range(c_n):
        pick_out[c] = jnp.where(views[c], sides[1], sides[0])
    to_crops(lambda peer: pick_out.at[peer], pick_in.at[my_c], ca_s, ca_r)
    pick_in[my_c] = pick_out[my_c]
    await_bytes(pick_in, c_n - 1, ca_r)

    chosen = pick_in[...].reshape(images, ROWS)
    back = (weights * 10.0) * (grad_ref[...] - chosen)
    cross = jnp.sum(unit * chosen, axis=1, keepdims=True) * 10.0
    along = jnp.sum(x * back, axis=1, keepdims=True)
    grad_ref[...] = norm * back - norm * norm * norm * x * along
    losses = jnp.broadcast_to(jnp.log(totals) - cross, (images, images))
    eye = lane[:, :images] == row[:, :images]
    loss_ref[...] = jnp.sum(jnp.where(eye, losses, 0.0), axis=0, keepdims=True)

    for ref, n, sem in (
        (su, y_n - 1, tu_s), (su, y_n - 1, th_s),
        (su, c_n // 2 - 1, su_s), (su, c_n // 2, sh_s), (pairs, c_n - 1, pr_s),
        (r1p, c_n - 1, r1p_s), (r1z, z_n - 1, r1z_s),
        (r2p, c_n - 1, r2p_s), (r2z, z_n - 1, r2z_s), (tot_p, c_n - 1, tp_s),
        (tot_z, z_n - 1, tz_s), (a_in, c_n - 1, a_s),
        (az_in, z_n - 1, az_s), (a_all, z_n - 1, ag_s), (ct_in, c_n - 1, ct_s),
        (cz_in, z_n - 1, cz_s), (c_tiles, 7, cg_s), (pick_in, c_n - 1, ca_s),
        (r3p, c_n - 1, r3p_s), (r3z, z_n - 1, r3z_s),
    ):
        await_bytes(ref, n, sem)


def solution(mesh):
    y_n, c_n, z_n = (mesh.shape[a] for a in ("image", "crop", "proto"))

    def step(teacher_feats, student_feats, teacher_protos, student_protos, pairing, row_weight):
        images, views, width = teacher_feats.shape
        vmem = pl.BlockSpec(memory_space=pltpu.VMEM)
        hbm = pl.BlockSpec(memory_space=pl.ANY)
        dma = pltpu.SemaphoreType.DMA
        ram = pltpu.VMEM
        grad, loss = pl.pallas_call(
            functools.partial(kernel, y_n, c_n, z_n),
            out_shape=(
                jax.ShapeDtypeStruct((images, width), F32),
                jax.ShapeDtypeStruct((1, images), F32),
            ),
            in_specs=[hbm] * 6,
            out_specs=(vmem, vmem),
            scratch_shapes=[
                ram((images, views, width), BF16),
                ram((images, width), BF16),
                ram((1, images), jnp.int32),
                ram((1, images), BF16),
                ram((width, COLS), BF16),
                ram((width, COLS), BF16),
                ram((width, COLS), BF16),
                ram((width, COLS), BF16),
                ram((ROWS, COLS), F32),
                ram((ROWS, COLS), BF16),
                ram((y_n, views, images, width), BF16),
                ram((c_n, images, width), BF16),
                ram((ROWS, LANES), F32),
                ram((ROWS, LANES), F32),
                ram((ROWS, LANES), F32),
                ram((8, COLS), F32),
                ram((8, COLS), F32),
                ram((c_n, 4, LANES), F32),
                ram((z_n, 4, LANES), BF16),
                ram((c_n, 4, LANES), F32),
                ram((z_n, 4, LANES), BF16),
                ram((c_n, 4, LANES), F32),
                ram((4, 1, LANES), F32),
                ram((z_n, 1, LANES), F32),
                ram((c_n, 1, images), F32),
                ram((c_n, images, width), BF16),
                ram((c_n, images, width), BF16),
                ram((z_n, 8, 256), BF16),
                ram((z_n, 8, 256), BF16),
                ram((z_n, 8, 256), F32),
                ram((c_n, 2, 8, width), BF16),
                ram((c_n, 2, 8, width), BF16),
                ram((8, 8, LANES), BF16),
                ram((z_n, 8, LANES), BF16),
                ram((8, 8, LANES), F32),
                ram((c_n, 8, width), F32),
                ram((c_n, 8, width), F32),
                ram((c_n, 1, LANES), F32),
                ram((z_n, 1, LANES), F32),
                dma((6,)),
                dma((y_n,)),
                dma((y_n,)),
            ]
            + [dma(())] * 38,
            compiler_params=pltpu.CompilerParams(collective_id=0, has_side_effects=True),
        )(
            teacher_feats,
            student_feats.reshape(images, width),
            pairing,
            row_weight,
            teacher_protos,
            student_protos,
        )
        return grad.reshape(1, images, width), loss

    return jax.shard_map(
        step,
        mesh=mesh,
        in_specs=(
            P("image", None, None),
            P("crop", "image", None),
            P(None, ("crop", "proto")),
            P(None, ("crop", "proto")),
            P("crop", "image"),
            P("crop", "image"),
        ),
        out_specs=(P("crop", "image", None), P("crop", "image")),
        check_vma=False,
    )
```

```python
import functools

import jax
import jax.numpy as jnp
from jax import lax
from jax.experimental import pallas as pl
from jax.experimental.pallas import tpu as pltpu
from jax.sharding import PartitionSpec as P

EPSILON = 1e-06
LOG2_E = 1.4426950408889634
TEACHER = 25.0 * LOG2_E
STUDENT = 10.0 * LOG2_E
MESH = pl.DeviceIdType.MESH
F32 = jnp.float32
BF16 = jnp.bfloat16
NT = (((1,), (1,)), ((), ()))
ROWS = 512
COLS = 2048
LANES = 128
CHUNK = 256


def every(n, body):
    lax.fori_loop(0, n, lambda k, c: (body(k), c)[1], 0)


def unit_rows(x):
    return x * lax.rsqrt(jnp.sum(x * x, axis=1, keepdims=True) + EPSILON)


def column_scales(raw, out):
    def chunk(j, carry):
        cols = pl.ds(pl.multiple_of(j * LANES, LANES), LANES)
        sums = jnp.zeros((8, LANES), F32)
        for r in range(8):
            w = raw[64 * r : 64 * r + 64, cols].astype(F32)
            sums = sums + jnp.sum((w * w).reshape(8, 8, LANES), axis=0)
        scale = lax.rsqrt(jnp.sum(sums, axis=0, keepdims=True) + EPSILON)
        out[:, cols] = jnp.broadcast_to(scale, (8, LANES))
        return carry

    lax.fori_loop(0, COLS // LANES, chunk, 0, unroll=4)


def lane_sums(ref, groups):
    sums = [
        jnp.sum(ref[q * LANES : (q + 1) * LANES, :].T, axis=0, keepdims=True) for q in range(groups)
    ]
    return jnp.concatenate(sums, axis=0) if groups > 1 else sums[0]


def kernel(
    y_n, c_n, z_n,
    tf_hbm, sf_hbm, pair_hbm, weight_hbm, tp_hbm, sp_hbm,
    grad_ref, loss_ref,
    tf, sf, pair, weight, tp, sp, t_scale, s_scale, t, e, tu, su, part, spart, ubuf, v, csum,
    r1p, r1z, r2p, r2z, tot_p, tot_sum, tot_z, pairs,
    a_out, a_in, az_out, az_in, a_all,
    ct_out, ct_in, cz_out, cz_in, c_tiles, pick_out, pick_in, r3p, r3z,
    load, tu_r, th_r,
    tu_s, th_s, su_s, su_r, sh_s, sh_r, pr_s, pr_r, r1p_s, r1p_r, r1z_s, r1z_r,
    r2p_s, r2p_r, r2z_s, r2z_r, tp_s, tp_r, tz_s, tz_r, a_s, a_r, az_s, az_r, ag_s, ag_r,
    ct_s, ct_r, cz_s, cz_r, cg_s, cg_r, ca_s, ca_r, r3p_s, r3p_r, r3z_s, r3z_r,
):
    my_y, my_c, my_z = (lax.axis_index(a) for a in ("image", "crop", "proto"))
    side = lax.rem(my_c, 2)
    partner = my_c + 1 - 2 * side

    loads = [
        pltpu.make_async_copy(src, dst, load.at[k])
        for k, (src, dst) in enumerate(
            ((tf_hbm, tf), (sf_hbm, sf), (tp_hbm, tp), (sp_hbm, sp), (pair_hbm, pair), (weight_hbm, weight))
        )
    ]
    for copy in loads:
        copy.start()

    def far_first(k):
        step = k + 1
        return z_n // 2 + (1 - 2 * lax.rem(step, 2)) * (step // 2)

    def push(src, dst, sends, recvs, axis, peer):
        pltpu.make_async_remote_copy(
            src_ref=src, dst_ref=dst, send_sem=sends, recv_sem=recvs,
            device_id={axis: peer}, device_id_type=MESH,
        ).start()

    def to_crops(src, dst, sends, recvs):
        def one(k):
            peer = lax.rem(my_c + k + 1, c_n)
            push(src(peer), dst, sends, recvs, "crop", peer)

        every(c_n - 1, one)

    def to_protos(src, dst, sends, recvs):
        def one(k):
            peer = lax.rem(my_z + far_first(k), z_n)
            push(src(peer), dst, sends, recvs, "proto", peer)

        every(z_n - 1, one)

    def await_bytes(ref, n, sem):
        some = ref.at[pl.ds(0, n)]
        pltpu.make_async_copy(some, some, sem).wait()

    barrier = pltpu.get_barrier_semaphore()

    def greet(axis, me, n):
        def one(k):
            pl.semaphore_signal(
                barrier, inc=1, device_id={axis: lax.rem(me + k + 1, n)}, device_id_type=MESH
            )

        every(n - 1, one)

    greet("proto", my_z, z_n)
    greet("image", my_y, y_n)
    greet("crop", my_c, c_n)

    loads[0].wait()
    for g in range(2):
        tu[my_y, g] = unit_rows(tf[:, g, :].astype(F32)).astype(BF16)
    loads[1].wait()
    su[my_c] = unit_rows(sf[...].astype(F32)).astype(BF16)
    loads[4].wait()
    pairs[my_c] = pair[...].astype(F32)
    loads[2].wait()
    column_scales(tp, t_scale)

    pl.semaphore_wait(barrier, y_n + c_n + z_n - 3)

    def give_rows(k):
        peer = lax.rem(my_y + 2 * k + 1 - 3 * (k // 2), y_n)
        push(tu.at[my_y, side], tu.at[my_y, side], tu_s, tu_r.at[my_y], "image", peer)

    every(y_n - 1, give_rows)

    def give_students(k):
        peer = lax.rem(my_c + 2 * k + 2, c_n)
        push(su.at[my_c], su.at[my_c], su_s, su_r, "crop", peer)

    every(c_n // 2 - 1, give_students)
    push(su.at[my_c], su.at[my_c], sh_s, sh_r, "crop", partner)
    to_crops(lambda peer: pairs.at[my_c], pairs.at[my_c], pr_s, pr_r)

    def transport(y, first):
        def chunk(i):
            for k in range(4):
                cols = pl.ds(pl.multiple_of((i * 4 + k) * CHUNK, CHUNK), CHUNK)
                rows = tu[y].reshape(LANES, ROWS)
                product = jnp.dot(rows, tp[:, cols], preferred_element_type=F32)
                terms = jnp.exp2(product * (t_scale[0:1, cols] * TEACHER))
                t[pl.ds(pl.multiple_of(y * LANES, LANES), LANES), cols] = terms
                sums = jnp.sum(terms.reshape(LANES // 8, 8, CHUNK), axis=0)
                csum[:, cols] = sums if first else csum[:, cols] + sums

        every(2, chunk)

    def hand_over(y):
        pltpu.make_async_copy(tu.at[y, side], tu.at[y, side], tu_r.at[y]).wait()
        push(tu.at[y, side], tu.at[y, side], th_s, th_r.at[y], "crop", partner)

    def handed(y):
        pltpu.make_async_copy(tu.at[y, side], tu.at[y, side], th_r.at[y]).wait()

    others = [lax.rem(my_y + k, y_n) for k in (1, 3, 2)]
    transport(my_y, True)
    loads[3].wait()
    column_scales(sp, s_scale)
    hand_over(others[0])
    hand_over(others[1])
    handed(others[0])
    transport(others[0], False)
    hand_over(others[2])
    await_bytes(su, c_n // 2 - 1, su_r)

    def hand_students(k):
        slot = lax.rem(my_c + 2 * k + 2, c_n)
        push(su.at[slot], su.at[slot], sh_s, sh_r, "crop", partner)

    every(c_n // 2 - 1, hand_students)
    handed(others[1])
    transport(others[1], False)
    handed(others[2])
    transport(others[2], False)

    def set_v(sums):
        for k, s in enumerate(sums):
            v[:, k * LANES : (k + 1) * LANES] = jnp.broadcast_to(
                1.0 / jnp.sum(s, axis=0, keepdims=True), (8, LANES)
            )

    set_v([csum[:, k * LANES : (k + 1) * LANES] for k in range(COLS // LANES)])

    def row_pass():
        def block(r, carry):
            rows = pl.ds(pl.multiple_of(r * 8, 8), 8)
            total = t[rows, 0:LANES] * v[:, 0:LANES]
            for k in range(1, COLS // LANES):
                cols = slice(k * LANES, (k + 1) * LANES)
                total = total + t[rows, cols] * v[:, cols]
            part[rows, :] = total
            return carry

        lax.fori_loop(0, ROWS // 8, block, 0, unroll=4)
        return lane_sums(part, 4)

    def column_pass(row_sums):
        u = 1.0 / row_sums
        for q in range(ROWS // LANES):
            ubuf[q * LANES : (q + 1) * LANES, :] = jnp.broadcast_to(u[q : q + 1, :], (LANES, LANES)).T

        def block(r, sums):
            rows = pl.ds(pl.multiple_of(r * 8, 8), 8)
            scale = ubuf[rows, :]
            return tuple(
                s + t[rows, k * LANES : (k + 1) * LANES] * scale for k, s in enumerate(sums)
            )

        zero = tuple(jnp.zeros((8, LANES), F32) for _ in range(COLS // LANES))
        set_v(lax.fori_loop(0, ROWS // 8, block, zero, unroll=4))

    r1p[my_c] = row_pass()
    to_crops(lambda peer: r1p.at[my_c], r1p.at[my_c], r1p_s, r1p_r)

    await_bytes(su, c_n // 2, sh_r)
    spart[...] = jnp.zeros_like(spart)

    def student(i):
        for k in range(2):
            cols = pl.ds(pl.multiple_of((2 * i + k) * CHUNK, CHUNK), CHUNK)
            for h in range(2):
                some = slice(256 * h, 256 * h + 256)
                rows = su[4 * h : 4 * h + 4].reshape(256, ROWS)
                product = jnp.dot(rows, sp[:, cols], preferred_element_type=F32)
                scale = s_scale[0:1, cols]
                terms = jnp.exp2(product * (scale * STUDENT))
                spart[some, :] += terms[:, :LANES] + terms[:, LANES:]
                e[some, cols] = (terms * scale).astype(BF16)

    every(COLS // CHUNK // 2, student)

    await_bytes(r1p, c_n - 1, r1p_r)
    r1z[my_z] = jnp.sum(r1p[...], axis=0).astype(BF16)
    to_protos(lambda peer: r1z.at[my_z], r1z.at[my_z], r1z_s, r1z_r)

    for j in range(2):
        some = slice(j * CHUNK, (j + 1) * CHUNK)
        back = lax.dot_general(e[...], sp[some, :], NT, preferred_element_type=F32)
        a_out[:, :, some] = back.astype(BF16).reshape(c_n, ROWS // c_n, CHUNK)
    to_crops(lambda peer: a_out.at[peer], a_in.at[my_c], a_s, a_r)
    tot_p[my_c] = lane_sums(spart, 4)
    to_crops(lambda peer: tot_p.at[my_c], tot_p.at[my_c], tp_s, tp_r)

    await_bytes(r1z, z_n - 1, r1z_r)
    column_pass(jnp.sum(r1z[...].astype(F32), axis=0))
    r2p[my_c] = row_pass()
    to_crops(lambda peer: r2p.at[my_c], r2p.at[my_c], r2p_s, r2p_r)

    await_bytes(r2p, c_n - 1, r2p_r)
    r2z[my_z] = jnp.sum(r2p[...], axis=0).astype(BF16)
    to_protos(lambda peer: r2z.at[my_z], r2z.at[my_z], r2z_s, r2z_r)
    await_bytes(a_in, c_n - 1, a_r)
    a_in[my_c] = a_out[my_c]
    for g in range(8):
        rows = slice(g * 8, g * 8 + 8)
        total = a_in[0, rows, :].astype(F32)
        for k in range(1, c_n):
            total = total + a_in[k, rows, :].astype(F32)
        for h in range(2):
            az_out[2 * g + h] = total[:, h * 256 : (h + 1) * 256].astype(BF16)
    await_bytes(tot_p, c_n - 1, tp_r)
    whole = jnp.sum(tot_p[...], axis=0)
    for q in range(4):
        tot_sum[q] = whole[q : q + 1, :]
    tot_z[my_z] = tot_sum[my_c // 2]

    to_protos(lambda peer: az_out.at[peer], az_in.at[my_z], az_s, az_r)
    to_protos(lambda peer: tot_z.at[my_z], tot_z.at[my_z], tz_s, tz_r)

    await_bytes(r2z, z_n - 1, r2z_r)
    column_pass(jnp.sum(r2z[...].astype(F32), axis=0))

    own_rows = pl.ds(pl.multiple_of(my_y * LANES, LANES), LANES)
    for k in range(COLS // CHUNK):
        cols = slice(k * CHUNK, (k + 1) * CHUNK)
        scaled = t[own_rows, cols] * v[0:1, cols]
        e[0:LANES, cols] = (scaled * s_scale[0:1, cols]).astype(BF16)
        halves = scaled[:, :LANES] + scaled[:, LANES:]
        part[0:LANES, :] = halves if k == 0 else part[0:LANES, :] + halves
    r3p[my_c] = lane_sums(part, 1)
    to_crops(lambda peer: r3p.at[my_c], r3p.at[my_c], r3p_s, r3p_r)
    sums = lax.dot_general(e[0:LANES, :], sp[...], NT, preferred_element_type=F32)
    for c in range(c_n):
        for g in range(2):
            ct_out[c, g] = sums[64 * g + 8 * c : 64 * g + 8 * c + 8, :].astype(BF16)
    to_crops(lambda peer: ct_out.at[peer], ct_in.at[my_c], ct_s, ct_r)
    ct_in[my_c] = ct_out[my_c]

    await_bytes(az_in, z_n - 1, az_r)
    az_in[my_z] = az_out[my_z]
    a_all[my_z] = jnp.sum(az_in[...].astype(F32), axis=0)
    to_protos(lambda peer: a_all.at[my_z], a_all.at[my_z], ag_s, ag_r)

    await_bytes(r3p, c_n - 1, r3p_r)
    r3z[my_z] = jnp.sum(r3p[...], axis=0)
    to_protos(lambda peer: r3z.at[my_z], r3z.at[my_z], r3z_s, r3z_r)
    await_bytes(ct_in, c_n - 1, ct_r)
    total = jnp.sum(ct_in[...].astype(F32), axis=0)
    for g in range(2):
        for k in range(4):
            cz_out[4 * g + k] = total[g, :, k * LANES : (k + 1) * LANES].astype(BF16)
    to_protos(lambda peer: cz_out.at[lax.rem(peer, 8)], cz_in.at[my_z], cz_s, cz_r)
    cz_in[my_z] = cz_out[lax.rem(my_z, 8)]

    images = ROWS // c_n
    lane = lax.broadcasted_iota(jnp.int32, (images, LANES), 1)
    row = lax.broadcasted_iota(jnp.int32, (images, LANES), 0)

    def as_column(values, first, rows):
        n = values.shape[1]
        wide = jnp.broadcast_to(values, (rows, n))
        picked = jnp.where(lane[:rows, :n] == row[:rows, :n] + first, wide, jnp.zeros_like(wide))
        return jnp.sum(picked, axis=1, keepdims=True)

    loads[5].wait()
    weights = as_column(weight[...].astype(F32), 0, images)
    x = sf[...].astype(F32)
    unit = su[my_c].astype(F32)
    norm = lax.rsqrt(jnp.sum(x * x, axis=1, keepdims=True) + EPSILON)
    await_bytes(pairs, c_n - 1, pr_r)
    views = [as_column(pairs[c], my_c * 8, 8) > 0.5 for c in range(c_n)]
    await_bytes(tot_z, z_n - 1, tz_r)
    totals = as_column(jnp.sum(tot_z[...], axis=0), side * images, images)
    await_bytes(r3z, z_n - 1, r3z_r)
    last = 1.0 / jnp.sum(r3z[...], axis=0)
    scales = [as_column(last, images * g + my_c * 8, 8) for g in range(2)]

    await_bytes(cz_in, z_n - 1, cz_r)
    mine = lax.rem(my_z, 8)
    c_tiles[mine] = jnp.sum(cz_in[...].astype(F32), axis=0)

    def near(k):
        offset = k + z_n - 4 + jnp.where(k >= 4, 1, 0)
        peer = lax.rem(my_z + offset, z_n)
        push(c_tiles.at[mine], c_tiles.at[mine], cg_s, cg_r, "proto", peer)

    every(7, near)
    await_bytes(a_all, z_n - 1, ag_r)
    for g in range(8):
        for h in range(2):
            grad_ref[g * 8 : g * 8 + 8, h * 256 : (h + 1) * 256] = a_all[2 * g + h] / totals[g * 8 : g * 8 + 8]

    await_bytes(c_tiles, 7, cg_r)
    sides = [
        jnp.concatenate([c_tiles[4 * g + k] for k in range(4)], axis=1) * scales[g] for g in range(2)
    ]
    for c in range(c_n):
        pick_out[c] = jnp.where(views[c], sides[1], sides[0])
    to_crops(lambda peer: pick_out.at[peer], pick_in.at[my_c], ca_s, ca_r)
    pick_in[my_c] = pick_out[my_c]
    await_bytes(pick_in, c_n - 1, ca_r)

    chosen = pick_in[...].reshape(images, ROWS)
    back = (weights * 10.0) * (grad_ref[...] - chosen)
    cross = jnp.sum(unit * chosen, axis=1, keepdims=True) * 10.0
    along = jnp.sum(x * back, axis=1, keepdims=True)
    grad_ref[...] = norm * back - norm * norm * norm * x * along
    losses = jnp.broadcast_to(jnp.log(totals) - cross, (images, images))
    eye = lane[:, :images] == row[:, :images]
    loss_ref[...] = jnp.sum(jnp.where(eye, losses, 0.0), axis=0, keepdims=True)

    for ref, n, sem in (
        (su, y_n - 1, tu_s), (su, y_n - 1, th_s),
        (su, c_n // 2 - 1, su_s), (su, c_n // 2, sh_s), (pairs, c_n - 1, pr_s),
        (r1p, c_n - 1, r1p_s), (r1z, z_n - 1, r1z_s),
        (r2p, c_n - 1, r2p_s), (r2z, z_n - 1, r2z_s), (tot_p, c_n - 1, tp_s),
        (tot_z, z_n - 1, tz_s), (a_in, c_n - 1, a_s),
        (az_in, z_n - 1, az_s), (a_all, z_n - 1, ag_s), (ct_in, c_n - 1, ct_s),
        (cz_in, z_n - 1, cz_s), (c_tiles, 7, cg_s), (pick_in, c_n - 1, ca_s),
        (r3p, c_n - 1, r3p_s), (r3z, z_n - 1, r3z_s),
    ):
        await_bytes(ref, n, sem)


def deliver(grad_in, loss_in, grad_ref, loss_ref):
    grad_ref[0] = grad_in[...]
    loss_ref[...] = loss_in[...]


def solution(mesh):
    y_n, c_n, z_n = (mesh.shape[a] for a in ("image", "crop", "proto"))

    def step(teacher_feats, student_feats, teacher_protos, student_protos, pairing, row_weight):
        images, views, width = teacher_feats.shape
        vmem = pl.BlockSpec(memory_space=pltpu.VMEM)
        hbm = pl.BlockSpec(memory_space=pltpu.HBM)
        dma = pltpu.SemaphoreType.DMA
        ram = pltpu.VMEM
        grad, loss = pl.pallas_call(
            functools.partial(kernel, y_n, c_n, z_n),
            out_shape=(
                jax.ShapeDtypeStruct((images, width), F32),
                jax.ShapeDtypeStruct((1, images), F32),
            ),
            in_specs=[hbm] * 6,
            out_specs=(vmem, vmem),
            scratch_shapes=[
                ram((images, views, width), BF16),
                ram((images, width), BF16),
                ram((1, images), jnp.int32),
                ram((1, images), BF16),
                ram((width, COLS), BF16),
                ram((width, COLS), BF16),
                ram((8, COLS), F32),
                ram((8, COLS), F32),
                ram((ROWS, COLS), F32),
                ram((ROWS, COLS), BF16),
                ram((y_n, views, images, width), BF16),
                ram((c_n, images, width), BF16),
                ram((ROWS, LANES), F32),
                ram((ROWS, LANES), F32),
                ram((ROWS, LANES), F32),
                ram((8, COLS), F32),
                ram((8, COLS), F32),
                ram((c_n, 4, LANES), F32),
                ram((z_n, 4, LANES), BF16),
                ram((c_n, 4, LANES), F32),
                ram((z_n, 4, LANES), BF16),
                ram((c_n, 4, LANES), F32),
                ram((4, 1, LANES), F32),
                ram((z_n, 1, LANES), F32),
                ram((c_n, 1, images), F32),
                ram((c_n, images, width), BF16),
                ram((c_n, images, width), BF16),
                ram((z_n, 8, 256), BF16),
                ram((z_n, 8, 256), BF16),
                ram((z_n, 8, 256), F32),
                ram((c_n, 2, 8, width), BF16),
                ram((c_n, 2, 8, width), BF16),
                ram((8, 8, LANES), BF16),
                ram((z_n, 8, LANES), BF16),
                ram((8, 8, LANES), F32),
                ram((c_n, 8, width), F32),
                ram((c_n, 8, width), F32),
                ram((c_n, 1, LANES), F32),
                ram((z_n, 1, LANES), F32),
                dma((6,)),
                dma((y_n,)),
                dma((y_n,)),
            ]
            + [dma(())] * 38,
            compiler_params=pltpu.CompilerParams(
                collective_id=0, has_side_effects=True, vmem_limit_bytes=32 * 1024 * 1024
            ),
        )(
            *(
                pltpu.with_memory_space_constraint(x, pltpu.HBM)
                for x in (
                    teacher_feats,
                    student_feats.reshape(images, width),
                    pairing,
                    row_weight,
                    teacher_protos,
                    student_protos,
                )
            )
        )
        return pl.pallas_call(
            deliver,
            out_shape=(
                jax.ShapeDtypeStruct((1, images, width), F32),
                jax.ShapeDtypeStruct((1, images), F32),
            ),
            in_specs=[vmem] * 2,
            out_specs=(vmem, vmem),
            compiler_params=pltpu.CompilerParams(vmem_limit_bytes=2 * 1024 * 1024),
        )(grad, loss)

    return jax.shard_map(
        step,
        mesh=mesh,
        in_specs=(
            P("image", None, None),
            P("crop", "image", None),
            P(None, ("crop", "proto")),
            P(None, ("crop", "proto")),
            P("crop", "image"),
            P("crop", "image"),
        ),
        out_specs=(P("crop", "image", None), P("crop", "image")),
        check_vma=False,
    )
```

```python
import functools

import jax
import jax.numpy as jnp
from jax import lax
from jax.experimental import pallas as pl
from jax.experimental.pallas import tpu as pltpu
from jax.sharding import PartitionSpec as P

EPSILON = 1e-06
LOG2_E = 1.4426950408889634
TEACHER = 25.0 * LOG2_E
STUDENT = 10.0 * LOG2_E
MESH = pl.DeviceIdType.MESH
F32 = jnp.float32
BF16 = jnp.bfloat16
NT = (((1,), (1,)), ((), ()))
ROWS = 512
COLS = 2048
LANES = 128
CHUNK = 256


def every(n, body):
    lax.fori_loop(0, n, lambda k, c: (body(k), c)[1], 0)


def unit_rows(x):
    return x * lax.rsqrt(jnp.sum(x * x, axis=1, keepdims=True) + EPSILON)


def column_scales(raw, out):
    def chunk(j, carry):
        cols = pl.ds(pl.multiple_of(j * LANES, LANES), LANES)
        sums = jnp.zeros((8, LANES), F32)
        for r in range(8):
            w = raw[64 * r : 64 * r + 64, cols].astype(F32)
            sums = sums + jnp.sum((w * w).reshape(8, 8, LANES), axis=0)
        scale = lax.rsqrt(jnp.sum(sums, axis=0, keepdims=True) + EPSILON)
        out[:, cols] = jnp.broadcast_to(scale, (8, LANES))
        return carry

    lax.fori_loop(0, COLS // LANES, chunk, 0, unroll=4)


def lane_sums(ref, groups):
    sums = [
        jnp.sum(ref[q * LANES : (q + 1) * LANES, :].T, axis=0, keepdims=True) for q in range(groups)
    ]
    return jnp.concatenate(sums, axis=0) if groups > 1 else sums[0]


def kernel(
    y_n, c_n, z_n,
    tf_hbm, sf_hbm, pair_hbm, weight_hbm, tp_hbm, sp_hbm,
    grad_ref, loss_ref,
    tf, sf, pair, weight, tp, sp, t_scale, s_scale, t, e, tu, su, part, spart, ubuf, v, csum,
    r1p, r1z, r2p, r2z, tot_p, tot_sum, tot_z, pairs,
    a_out, a_mid, a_pre, a_in, az_out, az_in, a_all, col_sums,
    ct_out, ct_in, cz_out, cz_in, c_tiles, pick_out, pick_in, r3p, r3z,
    load, tu_r, th_r,
    tu_s, th_s, su_s, su_r, sh_s, sh_r, pr_s, pr_r, r1p_s, r1p_r, r1z_s, r1z_r,
    r2p_s, r2p_r, r2z_s, r2z_r, tp_s, tp_r, tz_s, tz_r, a_s, a_r, az_s, az_r, ag_s, ag_r,
    am_s, am_r, cs_s, cs_r, ct_s, ct_r, cz_s, cz_r, cg_s, cg_r, ca_s, ca_r, r3p_s, r3p_r, r3z_s, r3z_r,
):
    my_y, my_c, my_z = (lax.axis_index(a) for a in ("image", "crop", "proto"))
    side = lax.rem(my_c, 2)
    partner = my_c + 1 - 2 * side

    loads = [
        pltpu.make_async_copy(src, dst, load.at[k])
        for k, (src, dst) in enumerate(
            ((tf_hbm, tf), (sf_hbm, sf), (tp_hbm, tp), (sp_hbm, sp), (pair_hbm, pair), (weight_hbm, weight))
        )
    ]

    def far_first(k):
        step = k + 1
        return z_n // 2 + (1 - 2 * lax.rem(step, 2)) * (step // 2)

    def push(src, dst, sends, recvs, axis, peer):
        pltpu.make_async_remote_copy(
            src_ref=src, dst_ref=dst, send_sem=sends, recv_sem=recvs,
            device_id={axis: peer}, device_id_type=MESH,
        ).start()

    def to_crops(src, dst, sends, recvs):
        def one(k):
            peer = lax.rem(my_c + k + 1, c_n)
            push(src(peer), dst, sends, recvs, "crop", peer)

        every(c_n - 1, one)

    def to_protos(src, dst, sends, recvs):
        def one(k):
            peer = lax.rem(my_z + far_first(k), z_n)
            push(src(peer), dst, sends, recvs, "proto", peer)

        every(z_n - 1, one)

    def await_bytes(ref, n, sem):
        some = ref.at[pl.ds(0, n)]
        pltpu.make_async_copy(some, some, sem).wait()

    barrier = pltpu.get_barrier_semaphore()

    def greet(peer):
        pl.semaphore_signal(barrier, inc=1, device_id=peer, device_id_type=MESH)

    def plane_peer(k):
        return {
            "image": lax.rem(my_y + (k + 1) // c_n, y_n),
            "crop": lax.rem(my_c + lax.rem(k + 1, c_n), c_n),
        }

    every(z_n - 1, lambda k: greet({"proto": lax.rem(my_z + far_first(k), z_n)}))
    for copy in loads:
        copy.start()
    every(y_n * c_n - 1, lambda k: greet(plane_peer(k)))

    loads[0].wait()
    for g in range(2):
        tu[my_y, g] = unit_rows(tf[:, g, :].astype(F32)).astype(BF16)
    loads[1].wait()
    su[my_c] = unit_rows(sf[...].astype(F32)).astype(BF16)
    loads[4].wait()
    pairs[my_c] = pair[...].astype(F32)
    loads[2].wait()
    column_scales(tp, t_scale)

    def transport(y, own):
        def chunk(i):
            for k in range(4):
                cols = pl.ds(pl.multiple_of((i * 4 + k) * CHUNK, CHUNK), CHUNK)
                rows = tu[y].reshape(LANES, ROWS)
                product = jnp.dot(rows, tp[:, cols], preferred_element_type=F32)
                terms = jnp.exp2(product * (t_scale[0:1, cols] * TEACHER))
                t[pl.ds(pl.multiple_of(y * LANES, LANES), LANES), cols] = terms
                if own:
                    csum[:, cols] = jnp.sum(terms.reshape(LANES // 8, 8, CHUNK), axis=0)

        every(2, chunk)

    transport(my_y, True)
    for k in range(COLS // LANES):
        cols = slice(k * LANES, (k + 1) * LANES)
        col_sums[my_y, :, cols] = jnp.sum(csum[:, cols], axis=0, keepdims=True)
    loads[3].wait()
    column_scales(sp, s_scale)

    pl.semaphore_wait(barrier, y_n * c_n + z_n - 2)

    def give_sums(k):
        peer = lax.rem(my_y + 2 * k + 1 - 3 * (k // 2), y_n)
        push(col_sums.at[my_y], col_sums.at[my_y], cs_s, cs_r, "image", peer)

    every(y_n - 1, give_sums)

    def give_rows(k):
        peer = lax.rem(my_y + 2 * k + 1 - 3 * (k // 2), y_n)
        push(tu.at[my_y, side], tu.at[my_y, side], tu_s, tu_r.at[my_y], "image", peer)

    every(y_n - 1, give_rows)

    def give_students(k):
        peer = lax.rem(my_c + 2 * k + 2, c_n)
        push(su.at[my_c], su.at[my_c], su_s, su_r, "crop", peer)

    every(c_n // 2 - 1, give_students)
    push(su.at[my_c], su.at[my_c], sh_s, sh_r, "crop", partner)
    to_crops(lambda peer: pairs.at[my_c], pairs.at[my_c], pr_s, pr_r)

    def hand_over(y):
        pltpu.make_async_copy(tu.at[y, side], tu.at[y, side], tu_r.at[y]).wait()
        push(tu.at[y, side], tu.at[y, side], th_s, th_r.at[y], "crop", partner)

    def handed(y):
        pltpu.make_async_copy(tu.at[y, side], tu.at[y, side], th_r.at[y]).wait()

    def set_v(sums):
        for k, s in enumerate(sums):
            v[:, k * LANES : (k + 1) * LANES] = jnp.broadcast_to(
                1.0 / jnp.sum(s, axis=0, keepdims=True), (8, LANES)
            )

    def row_pass(first, n):
        def block(r, carry):
            rows = pl.ds(pl.multiple_of(first + r * 8, 8), 8)
            total = t[rows, 0:LANES] * v[:, 0:LANES]
            for k in range(1, COLS // LANES):
                cols = slice(k * LANES, (k + 1) * LANES)
                total = total + t[rows, cols] * v[:, cols]
            part[pl.ds(pl.multiple_of(r * 8, 8), 8), :] = total
            return carry

        lax.fori_loop(0, n // 8, block, 0, unroll=4)
        return lane_sums(part, n // LANES)

    def column_pass(row_sums):
        u = 1.0 / row_sums
        for q in range(ROWS // LANES):
            ubuf[q * LANES : (q + 1) * LANES, :] = jnp.broadcast_to(u[q : q + 1, :], (LANES, LANES)).T

        def block(r, sums):
            rows = pl.ds(pl.multiple_of(r * 8, 8), 8)
            scale = ubuf[rows, :]
            return tuple(
                s + t[rows, k * LANES : (k + 1) * LANES] * scale for k, s in enumerate(sums)
            )

        zero = tuple(jnp.zeros((8, LANES), F32) for _ in range(COLS // LANES))
        set_v(lax.fori_loop(0, ROWS // 8, block, zero, unroll=4))

    await_bytes(col_sums, y_n - 1, cs_r)
    v[...] = jnp.broadcast_to(1.0 / jnp.sum(col_sums[...], axis=0), (8, COLS))
    mine_1 = my_y * c_n + my_c
    r1p[mine_1] = row_pass(my_y * LANES, LANES)

    def give_first(k):
        pltpu.make_async_remote_copy(
            src_ref=r1p.at[mine_1], dst_ref=r1p.at[mine_1], send_sem=r1p_s, recv_sem=r1p_r,
            device_id=plane_peer(k), device_id_type=MESH,
        ).start()

    every(y_n * c_n - 1, give_first)

    others = [lax.rem(my_y + k, y_n) for k in (1, 3, 2)]
    hand_over(others[0])
    hand_over(others[1])
    handed(others[0])
    transport(others[0], False)
    hand_over(others[2])
    await_bytes(su, c_n // 2 - 1, su_r)

    def hand_students(k):
        slot = lax.rem(my_c + 2 * k + 2, c_n)
        push(su.at[slot], su.at[slot], sh_s, sh_r, "crop", partner)

    every(c_n // 2 - 1, hand_students)
    handed(others[1])
    transport(others[1], False)
    handed(others[2])
    transport(others[2], False)

    await_bytes(r1p, y_n * c_n - 1, r1p_r)
    firsts = [jnp.sum(r1p[c_n * y : c_n * y + c_n], axis=0) for y in range(y_n)]
    r1z[my_z] = jnp.concatenate(firsts, axis=0).astype(BF16)
    to_protos(lambda peer: r1z.at[my_z], r1z.at[my_z], r1z_s, r1z_r)

    await_bytes(su, c_n // 2, sh_r)
    spart[...] = jnp.zeros_like(spart)

    def student(i):
        for k in range(2):
            cols = pl.ds(pl.multiple_of((2 * i + k) * CHUNK, CHUNK), CHUNK)
            for h in range(2):
                some = slice(256 * h, 256 * h + 256)
                rows = su[4 * h : 4 * h + 4].reshape(256, ROWS)
                product = jnp.dot(rows, sp[:, cols], preferred_element_type=F32)
                scale = s_scale[0:1, cols]
                terms = jnp.exp2(product * (scale * STUDENT))
                spart[some, :] += terms[:, :LANES] + terms[:, LANES:]
                e[some, cols] = (terms * scale).astype(BF16)

    every(COLS // CHUNK // 2, student)

    for j in range(2):
        some = slice(j * CHUNK, (j + 1) * CHUNK)
        back = lax.dot_general(e[...], sp[some, :], NT, preferred_element_type=F32)
        for c in range(c_n):
            a_out[c % 2, c // 2, :, some] = back[64 * c : 64 * c + 64, :].astype(BF16)
    push(a_out.at[1 - side], a_mid, am_s, am_r, "crop", partner)
    tot_p[my_c] = lane_sums(spart, 4)
    to_crops(lambda peer: tot_p.at[my_c], tot_p.at[my_c], tp_s, tp_r)
    pltpu.make_async_copy(a_mid, a_mid, am_r).wait()
    my_x = my_c // 2

    def merge(x):
        a_pre[x] = (a_out[side, x].astype(F32) + a_mid[x].astype(F32)).astype(BF16)

    every(c_n // 2, merge)

    def give_parts(k):
        x = lax.rem(my_x + k + 1, c_n // 2)
        push(a_pre.at[x], a_in.at[my_x], a_s, a_r, "crop", 2 * x + side)

    every(c_n // 2 - 1, give_parts)

    await_bytes(r1z, z_n - 1, r1z_r)
    column_pass(jnp.sum(r1z[...].astype(F32), axis=0))
    r2p[my_c] = row_pass(0, ROWS)
    to_crops(lambda peer: r2p.at[my_c], r2p.at[my_c], r2p_s, r2p_r)

    await_bytes(r2p, c_n - 1, r2p_r)
    r2z[my_z] = jnp.sum(r2p[...], axis=0).astype(BF16)
    to_protos(lambda peer: r2z.at[my_z], r2z.at[my_z], r2z_s, r2z_r)
    await_bytes(a_in, c_n // 2 - 1, a_r)
    a_in[my_x] = a_pre[my_x]
    for g in range(8):
        rows = slice(g * 8, g * 8 + 8)
        total = a_in[0, rows, :].astype(F32)
        for k in range(1, c_n // 2):
            total = total + a_in[k, rows, :].astype(F32)
        for h in range(2):
            az_out[2 * g + h] = total[:, h * 256 : (h + 1) * 256].astype(BF16)
    await_bytes(tot_p, c_n - 1, tp_r)
    whole = jnp.sum(tot_p[...], axis=0)
    for q in range(4):
        tot_sum[q] = whole[q : q + 1, :]
    tot_z[my_z] = tot_sum[my_c // 2]

    to_protos(lambda peer: az_out.at[peer], az_in.at[my_z], az_s, az_r)
    to_protos(lambda peer: tot_z.at[my_z], tot_z.at[my_z], tz_s, tz_r)

    await_bytes(r2z, z_n - 1, r2z_r)
    column_pass(jnp.sum(r2z[...].astype(F32), axis=0))

    own_rows = pl.ds(pl.multiple_of(my_y * LANES, LANES), LANES)
    for k in range(COLS // CHUNK):
        cols = slice(k * CHUNK, (k + 1) * CHUNK)
        scaled = t[own_rows, cols] * v[0:1, cols]
        e[0:LANES, cols] = (scaled * s_scale[0:1, cols]).astype(BF16)
        halves = scaled[:, :LANES] + scaled[:, LANES:]
        part[0:LANES, :] = halves if k == 0 else part[0:LANES, :] + halves
    r3p[my_c] = lane_sums(part, 1)
    to_crops(lambda peer: r3p.at[my_c], r3p.at[my_c], r3p_s, r3p_r)
    sums = lax.dot_general(e[0:LANES, :], sp[...], NT, preferred_element_type=F32)
    for c in range(c_n):
        for g in range(2):
            ct_out[c, g] = sums[64 * g + 8 * c : 64 * g + 8 * c + 8, :].astype(BF16)
    to_crops(lambda peer: ct_out.at[peer], ct_in.at[my_c], ct_s, ct_r)
    ct_in[my_c] = ct_out[my_c]

    await_bytes(az_in, z_n - 1, az_r)
    az_in[my_z] = az_out[my_z]
    a_all[my_z] = jnp.sum(az_in[...].astype(F32), axis=0)
    to_protos(lambda peer: a_all.at[my_z], a_all.at[my_z], ag_s, ag_r)

    await_bytes(r3p, c_n - 1, r3p_r)
    r3z[my_z] = jnp.sum(r3p[...], axis=0)
    to_protos(lambda peer: r3z.at[my_z], r3z.at[my_z], r3z_s, r3z_r)
    await_bytes(ct_in, c_n - 1, ct_r)
    total = jnp.sum(ct_in[...].astype(F32), axis=0)
    for g in range(2):
        for k in range(4):
            cz_out[4 * g + k] = total[g, :, k * LANES : (k + 1) * LANES].astype(BF16)
    to_protos(lambda peer: cz_out.at[lax.rem(peer, 8)], cz_in.at[my_z], cz_s, cz_r)
    cz_in[my_z] = cz_out[lax.rem(my_z, 8)]

    images = ROWS // c_n
    lane = lax.broadcasted_iota(jnp.int32, (images, LANES), 1)
    row = lax.broadcasted_iota(jnp.int32, (images, LANES), 0)

    def as_column(values, first, rows):
        n = values.shape[1]
        wide = jnp.broadcast_to(values, (rows, n))
        picked = jnp.where(lane[:rows, :n] == row[:rows, :n] + first, wide, jnp.zeros_like(wide))
        return jnp.sum(picked, axis=1, keepdims=True)

    loads[5].wait()
    weights = as_column(weight[...].astype(F32), 0, images)
    x = sf[...].astype(F32)
    unit = su[my_c].astype(F32)
    norm = lax.rsqrt(jnp.sum(x * x, axis=1, keepdims=True) + EPSILON)
    await_bytes(pairs, c_n - 1, pr_r)
    views = [as_column(pairs[c], my_c * 8, 8) > 0.5 for c in range(c_n)]
    await_bytes(tot_z, z_n - 1, tz_r)
    totals = as_column(jnp.sum(tot_z[...], axis=0), side * images, images)
    await_bytes(r3z, z_n - 1, r3z_r)
    last = 1.0 / jnp.sum(r3z[...], axis=0)
    scales = [as_column(last, images * g + my_c * 8, 8) for g in range(2)]

    await_bytes(cz_in, z_n - 1, cz_r)
    mine = lax.rem(my_z, 8)
    c_tiles[mine] = jnp.sum(cz_in[...].astype(F32), axis=0)

    def near(k):
        offset = k + z_n - 4 + jnp.where(k >= 4, 1, 0)
        peer = lax.rem(my_z + offset, z_n)
        push(c_tiles.at[mine], c_tiles.at[mine], cg_s, cg_r, "proto", peer)

    every(7, near)
    await_bytes(a_all, z_n - 1, ag_r)
    for g in range(8):
        for h in range(2):
            grad_ref[g * 8 : g * 8 + 8, h * 256 : (h + 1) * 256] = a_all[2 * g + h] / totals[g * 8 : g * 8 + 8]

    await_bytes(c_tiles, 7, cg_r)
    sides = [
        jnp.concatenate([c_tiles[4 * g + k] for k in range(4)], axis=1) * scales[g] for g in range(2)
    ]
    for c in range(c_n):
        pick_out[c] = jnp.where(views[c], sides[1], sides[0])
    to_crops(lambda peer: pick_out.at[peer], pick_in.at[my_c], ca_s, ca_r)
    pick_in[my_c] = pick_out[my_c]
    await_bytes(pick_in, c_n - 1, ca_r)

    chosen = pick_in[...].reshape(images, ROWS)
    back = (weights * 10.0) * (grad_ref[...] - chosen)
    cross = jnp.sum(unit * chosen, axis=1, keepdims=True) * 10.0
    along = jnp.sum(x * back, axis=1, keepdims=True)
    grad_ref[...] = norm * back - norm * norm * norm * x * along
    losses = jnp.broadcast_to(jnp.log(totals) - cross, (images, images))
    eye = lane[:, :images] == row[:, :images]
    loss_ref[...] = jnp.sum(jnp.where(eye, losses, 0.0), axis=0, keepdims=True)

    for ref, n, sem in (
        (su, y_n - 1, tu_s), (su, y_n - 1, th_s), (col_sums, y_n - 1, cs_s),
        (su, c_n // 2 - 1, su_s), (su, c_n // 2, sh_s), (pairs, c_n - 1, pr_s),
        (r1p, y_n * c_n - 1, r1p_s), (r1z, z_n - 1, r1z_s),
        (r2p, c_n - 1, r2p_s), (r2z, z_n - 1, r2z_s), (tot_p, c_n - 1, tp_s),
        (tot_z, z_n - 1, tz_s), (a_in, c_n // 2 - 1, a_s),
        (az_in, z_n - 1, az_s), (a_all, z_n - 1, ag_s), (ct_in, c_n - 1, ct_s),
        (cz_in, z_n - 1, cz_s), (c_tiles, 7, cg_s), (pick_in, c_n - 1, ca_s),
        (r3p, c_n - 1, r3p_s), (r3z, z_n - 1, r3z_s),
    ):
        await_bytes(ref, n, sem)
    pltpu.make_async_copy(a_mid, a_mid, am_s).wait()


def deliver(grad_in, loss_in, grad_ref, loss_ref):
    grad_ref[0] = grad_in[...]
    loss_ref[...] = loss_in[...]


def solution(mesh):
    y_n, c_n, z_n = (mesh.shape[a] for a in ("image", "crop", "proto"))

    def step(teacher_feats, student_feats, teacher_protos, student_protos, pairing, row_weight):
        images, views, width = teacher_feats.shape
        vmem = pl.BlockSpec(memory_space=pltpu.VMEM)
        hbm = pl.BlockSpec(memory_space=pltpu.HBM)
        dma = pltpu.SemaphoreType.DMA
        ram = pltpu.VMEM
        grad, loss = pl.pallas_call(
            functools.partial(kernel, y_n, c_n, z_n),
            out_shape=(
                jax.ShapeDtypeStruct((images, width), F32),
                jax.ShapeDtypeStruct((1, images), F32),
            ),
            in_specs=[hbm] * 6,
            out_specs=(vmem, vmem),
            scratch_shapes=[
                ram((images, views, width), BF16),
                ram((images, width), BF16),
                ram((1, images), jnp.int32),
                ram((1, images), BF16),
                ram((width, COLS), BF16),
                ram((width, COLS), BF16),
                ram((8, COLS), F32),
                ram((8, COLS), F32),
                ram((ROWS, COLS), F32),
                ram((ROWS, COLS), BF16),
                ram((y_n, views, images, width), BF16),
                ram((c_n, images, width), BF16),
                ram((ROWS, LANES), F32),
                ram((ROWS, LANES), F32),
                ram((ROWS, LANES), F32),
                ram((8, COLS), F32),
                ram((8, COLS), F32),
                ram((y_n * c_n, 1, LANES), F32),
                ram((z_n, 4, LANES), BF16),
                ram((c_n, 4, LANES), F32),
                ram((z_n, 4, LANES), BF16),
                ram((c_n, 4, LANES), F32),
                ram((4, 1, LANES), F32),
                ram((z_n, 1, LANES), F32),
                ram((c_n, 1, images), F32),
                ram((2, c_n // 2, images, width), BF16),
                ram((c_n // 2, images, width), BF16),
                ram((c_n // 2, images, width), BF16),
                ram((c_n // 2, images, width), BF16),
                ram((z_n, 8, 256), BF16),
                ram((z_n, 8, 256), BF16),
                ram((z_n, 8, 256), F32),
                ram((y_n, 1, COLS), F32),
                ram((c_n, 2, 8, width), BF16),
                ram((c_n, 2, 8, width), BF16),
                ram((8, 8, LANES), BF16),
                ram((z_n, 8, LANES), BF16),
                ram((8, 8, LANES), F32),
                ram((c_n, 8, width), F32),
                ram((c_n, 8, width), F32),
                ram((c_n, 1, LANES), F32),
                ram((z_n, 1, LANES), F32),
                dma((6,)),
                dma((y_n,)),
                dma((y_n,)),
            ]
            + [dma(())] * 42,
            compiler_params=pltpu.CompilerParams(
                collective_id=0, has_side_effects=True, vmem_limit_bytes=32 * 1024 * 1024
            ),
        )(
            *(
                pltpu.with_memory_space_constraint(x, pltpu.HBM)
                for x in (
                    teacher_feats,
                    student_feats.reshape(images, width),
                    pairing,
                    row_weight,
                    teacher_protos,
                    student_protos,
                )
            )
        )
        return pl.pallas_call(
            deliver,
            out_shape=(
                jax.ShapeDtypeStruct((1, images, width), F32),
                jax.ShapeDtypeStruct((1, images), F32),
            ),
            in_specs=[vmem] * 2,
            out_specs=(vmem, vmem),
            compiler_params=pltpu.CompilerParams(vmem_limit_bytes=2 * 1024 * 1024),
        )(grad, loss)

    return jax.shard_map(
        step,
        mesh=mesh,
        in_specs=(
            P("image", None, None),
            P("crop", "image", None),
            P(None, ("crop", "proto")),
            P(None, ("crop", "proto")),
            P("crop", "image"),
            P("crop", "image"),
        ),
        out_specs=(P("crop", "image", None), P("crop", "image")),
        check_vma=False,
    )
```

```python
import functools

import jax
import jax.numpy as jnp
from jax import lax
from jax.experimental import pallas as pl
from jax.experimental.pallas import tpu as pltpu
from jax.sharding import PartitionSpec as P

EPSILON = 1e-06
LOG2_E = 1.4426950408889634
TEACHER = 25.0 * LOG2_E
STUDENT = 10.0 * LOG2_E
MESH = pl.DeviceIdType.MESH
F32 = jnp.float32
BF16 = jnp.bfloat16
NT = (((1,), (1,)), ((), ()))
ROWS = 512
COLS = 2048
LANES = 128
CHUNK = 256


def every(n, body):
    lax.fori_loop(0, n, lambda k, c: (body(k), c)[1], 0)


def unit_rows(x):
    return x * lax.rsqrt(jnp.sum(x * x, axis=1, keepdims=True) + EPSILON)


def column_scales(raw, out):
    def chunk(j, carry):
        cols = pl.ds(pl.multiple_of(j * LANES, LANES), LANES)
        sums = jnp.zeros((8, LANES), F32)
        for r in range(8):
            w = raw[64 * r : 64 * r + 64, cols].astype(F32)
            sums = sums + jnp.sum((w * w).reshape(8, 8, LANES), axis=0)
        scale = lax.rsqrt(jnp.sum(sums, axis=0, keepdims=True) + EPSILON)
        out[:, cols] = jnp.broadcast_to(scale, (8, LANES))
        return carry

    lax.fori_loop(0, COLS // LANES, chunk, 0, unroll=4)


def lane_sums(ref, groups):
    sums = [
        jnp.sum(ref[q * LANES : (q + 1) * LANES, :].T, axis=0, keepdims=True) for q in range(groups)
    ]
    return jnp.concatenate(sums, axis=0) if groups > 1 else sums[0]


def kernel(
    y_n, c_n, z_n,
    tf_hbm, sf_hbm, pair_hbm, weight_hbm, tp_hbm, sp_hbm,
    grad_ref, loss_ref,
    tf, sf, pair, weight, tp, sp, t_scale, s_scale, t, e, tu, su, part, spart, ubuf, v, csum,
    r1p, r1z, r2p, r2z, tot_p, tot_sum, tot_z, pairs,
    a_out, a_mid, a_pre, a_in, az_out, az_in, a_all, col_sums,
    ct_out, ct_in, cz_out, cz_in, pick_out, pick_in, r3p, r3z,
    load, tu_r, th_r,
    tu_s, th_s, su_s, su_r, sh_s, sh_r, pr_s, pr_r, r1p_s, r1p_r, r1z_s, r1z_r,
    r2p_s, r2p_r, r2z_s, r2z_r, tp_s, tp_r, tz_s, tz_r, a_s, a_r, az_s, az_r, ag_s, ag_r,
    am_s, am_r, cs_s, cs_r, ct_s, ct_r, cz_s, cz_r, ca_s, ca_r, r3p_s, r3p_r, r3z_s, r3z_r,
):
    my_y, my_c, my_z = (lax.axis_index(a) for a in ("image", "crop", "proto"))
    side = lax.rem(my_c, 2)
    partner = my_c + 1 - 2 * side

    loads = [
        pltpu.make_async_copy(src, dst, load.at[k])
        for k, (src, dst) in enumerate(
            ((tf_hbm, tf), (sf_hbm, sf), (tp_hbm, tp), (sp_hbm, sp), (pair_hbm, pair), (weight_hbm, weight))
        )
    ]

    def far_first(k):
        step = k + 1
        return z_n // 2 + (1 - 2 * lax.rem(step, 2)) * (step // 2)

    def push(src, dst, sends, recvs, axis, peer):
        pltpu.make_async_remote_copy(
            src_ref=src, dst_ref=dst, send_sem=sends, recv_sem=recvs,
            device_id={axis: peer}, device_id_type=MESH,
        ).start()

    def to_crops(src, dst, sends, recvs):
        def one(k):
            peer = lax.rem(my_c + lax.rem(k + 2, c_n - 1) + 1, c_n)
            push(src(peer), dst, sends, recvs, "crop", peer)

        every(c_n - 1, one)

    def to_protos(src, dst, sends, recvs):
        def one(k):
            peer = lax.rem(my_z + far_first(k), z_n)
            push(src(peer), dst, sends, recvs, "proto", peer)

        every(z_n - 1, one)

    def await_bytes(ref, n, sem):
        some = ref.at[pl.ds(0, n)]
        pltpu.make_async_copy(some, some, sem).wait()

    barrier = pltpu.get_barrier_semaphore()

    def greet(peer):
        pl.semaphore_signal(barrier, inc=1, device_id=peer, device_id_type=MESH)

    def plane_peer(k):
        step = lax.rem(k + 15, y_n * c_n - 1) + 1
        return {
            "image": lax.rem(my_y + step // c_n, y_n),
            "crop": lax.rem(my_c + lax.rem(step, c_n), c_n),
        }

    every(z_n - 1, lambda k: greet({"proto": lax.rem(my_z + far_first(k), z_n)}))
    for copy in loads:
        copy.start()
    every(y_n * c_n - 1, lambda k: greet(plane_peer(k)))

    loads[0].wait()
    for g in range(2):
        tu[my_y, g] = unit_rows(tf[:, g, :].astype(F32)).astype(BF16)
    loads[1].wait()
    su[my_c] = unit_rows(sf[...].astype(F32)).astype(BF16)
    loads[4].wait()
    pairs[my_c] = pair[...].astype(F32)
    loads[2].wait()
    column_scales(tp, t_scale)

    def transport(y, own):
        def chunk(i):
            for k in range(4):
                cols = pl.ds(pl.multiple_of((i * 4 + k) * CHUNK, CHUNK), CHUNK)
                rows = tu[y].reshape(LANES, ROWS)
                product = jnp.dot(rows, tp[:, cols], preferred_element_type=F32)
                terms = jnp.exp2(product * (t_scale[0:1, cols] * TEACHER))
                t[pl.ds(pl.multiple_of(y * LANES, LANES), LANES), cols] = terms
                if own:
                    csum[:, cols] = jnp.sum(terms.reshape(LANES // 8, 8, CHUNK), axis=0)

        every(2, chunk)

    transport(my_y, True)
    for k in range(COLS // LANES):
        cols = slice(k * LANES, (k + 1) * LANES)
        col_sums[my_y, :, cols] = jnp.sum(csum[:, cols], axis=0, keepdims=True)
    loads[3].wait()
    column_scales(sp, s_scale)

    pl.semaphore_wait(barrier, y_n * c_n + z_n - 2)

    def give_sums(k):
        peer = lax.rem(my_y + 2 - k + 3 * (k // 2), y_n)
        push(col_sums.at[my_y], col_sums.at[my_y], cs_s, cs_r, "image", peer)

    every(y_n - 1, give_sums)

    def give_rows(k):
        peer = lax.rem(my_y + 2 * k + 1 - 3 * (k // 2), y_n)
        push(tu.at[my_y, side], tu.at[my_y, side], tu_s, tu_r.at[my_y], "image", peer)

    every(y_n - 1, give_rows)

    def give_students(k):
        peer = lax.rem(my_c + 2 * k + 2, c_n)
        push(su.at[my_c], su.at[my_c], su_s, su_r, "crop", peer)

    every(c_n // 2 - 1, give_students)
    push(su.at[my_c], su.at[my_c], sh_s, sh_r, "crop", partner)
    to_crops(lambda peer: pairs.at[my_c], pairs.at[my_c], pr_s, pr_r)

    def hand_over(y):
        pltpu.make_async_copy(tu.at[y, side], tu.at[y, side], tu_r.at[y]).wait()
        push(tu.at[y, side], tu.at[y, side], th_s, th_r.at[y], "crop", partner)

    def handed(y):
        pltpu.make_async_copy(tu.at[y, side], tu.at[y, side], th_r.at[y]).wait()

    def set_v(sums):
        for k, s in enumerate(sums):
            v[:, k * LANES : (k + 1) * LANES] = jnp.broadcast_to(
                1.0 / jnp.sum(s, axis=0, keepdims=True), (8, LANES)
            )

    def row_pass(first, n):
        def block(r, carry):
            rows = pl.ds(pl.multiple_of(first + r * 8, 8), 8)
            total = t[rows, 0:LANES] * v[:, 0:LANES]
            for k in range(1, COLS // LANES):
                cols = slice(k * LANES, (k + 1) * LANES)
                total = total + t[rows, cols] * v[:, cols]
            part[pl.ds(pl.multiple_of(r * 8, 8), 8), :] = total
            return carry

        lax.fori_loop(0, n // 8, block, 0, unroll=4)
        return lane_sums(part, n // LANES)

    def column_pass(row_sums):
        u = 1.0 / row_sums
        for q in range(ROWS // LANES):
            ubuf[q * LANES : (q + 1) * LANES, :] = jnp.broadcast_to(u[q : q + 1, :], (LANES, LANES)).T

        def block(r, sums):
            rows = pl.ds(pl.multiple_of(r * 8, 8), 8)
            scale = ubuf[rows, :]
            return tuple(
                s + t[rows, k * LANES : (k + 1) * LANES] * scale for k, s in enumerate(sums)
            )

        zero = tuple(jnp.zeros((8, LANES), F32) for _ in range(COLS // LANES))
        set_v(lax.fori_loop(0, ROWS // 8, block, zero, unroll=4))

    await_bytes(col_sums, y_n - 1, cs_r)
    v[...] = jnp.broadcast_to(1.0 / jnp.sum(col_sums[...], axis=0), (8, COLS))
    mine_1 = my_y * c_n + my_c
    r1p[mine_1] = row_pass(my_y * LANES, LANES)

    def give_first(k):
        pltpu.make_async_remote_copy(
            src_ref=r1p.at[mine_1], dst_ref=r1p.at[mine_1], send_sem=r1p_s, recv_sem=r1p_r,
            device_id=plane_peer(k), device_id_type=MESH,
        ).start()

    every(y_n * c_n - 1, give_first)

    others = [lax.rem(my_y + k, y_n) for k in (1, 3, 2)]
    hand_over(others[0])
    hand_over(others[1])
    handed(others[0])
    transport(others[0], False)
    hand_over(others[2])
    await_bytes(su, c_n // 2 - 1, su_r)

    def hand_students(k):
        slot = lax.rem(my_c + 2 * k + 2, c_n)
        push(su.at[slot], su.at[slot], sh_s, sh_r, "crop", partner)

    every(c_n // 2 - 1, hand_students)
    handed(others[1])
    transport(others[1], False)
    handed(others[2])
    transport(others[2], False)

    await_bytes(r1p, y_n * c_n - 1, r1p_r)
    firsts = [jnp.sum(r1p[c_n * y : c_n * y + c_n], axis=0) for y in range(y_n)]
    r1z[my_z] = jnp.concatenate(firsts, axis=0).astype(BF16)
    to_protos(lambda peer: r1z.at[my_z], r1z.at[my_z], r1z_s, r1z_r)

    await_bytes(su, c_n // 2, sh_r)
    spart[...] = jnp.zeros_like(spart)

    def student(i):
        for k in range(2):
            cols = pl.ds(pl.multiple_of((2 * i + k) * CHUNK, CHUNK), CHUNK)
            for h in range(2):
                some = slice(256 * h, 256 * h + 256)
                rows = su[4 * h : 4 * h + 4].reshape(256, ROWS)
                product = jnp.dot(rows, sp[:, cols], preferred_element_type=F32)
                scale = s_scale[0:1, cols]
                terms = jnp.exp2(product * (scale * STUDENT))
                spart[some, :] += terms[:, :LANES] + terms[:, LANES:]
                e[some, cols] = (terms * scale).astype(BF16)

    every(COLS // CHUNK // 2, student)

    for j in range(2):
        some = slice(j * CHUNK, (j + 1) * CHUNK)
        back = lax.dot_general(e[...], sp[some, :], NT, preferred_element_type=F32)
        for c in range(c_n):
            a_out[c % 2, c // 2, :, some] = back[64 * c : 64 * c + 64, :].astype(BF16)
    push(a_out.at[1 - side], a_mid, am_s, am_r, "crop", partner)
    tot_p[my_c] = lane_sums(spart, 4)
    to_crops(lambda peer: tot_p.at[my_c], tot_p.at[my_c], tp_s, tp_r)
    pltpu.make_async_copy(a_mid, a_mid, am_r).wait()
    my_x = my_c // 2

    def merge(x):
        a_pre[x] = (a_out[side, x].astype(F32) + a_mid[x].astype(F32)).astype(BF16)

    every(c_n // 2, merge)

    def give_parts(k):
        x = lax.rem(my_x + k + 1, c_n // 2)
        push(a_pre.at[x], a_in.at[my_x], a_s, a_r, "crop", 2 * x + side)

    every(c_n // 2 - 1, give_parts)

    await_bytes(r1z, z_n - 1, r1z_r)
    column_pass(jnp.sum(r1z[...].astype(F32), axis=0))
    r2p[my_c] = row_pass(0, ROWS)
    to_crops(lambda peer: r2p.at[my_c], r2p.at[my_c], r2p_s, r2p_r)

    await_bytes(r2p, c_n - 1, r2p_r)
    r2z[my_z] = jnp.sum(r2p[...], axis=0).astype(BF16)
    to_protos(lambda peer: r2z.at[my_z], r2z.at[my_z], r2z_s, r2z_r)
    await_bytes(a_in, c_n // 2 - 1, a_r)
    a_in[my_x] = a_pre[my_x]
    for g in range(8):
        rows = slice(g * 8, g * 8 + 8)
        total = a_in[0, rows, :].astype(F32)
        for k in range(1, c_n // 2):
            total = total + a_in[k, rows, :].astype(F32)
        for h in range(2):
            az_out[2 * g + h] = total[:, h * 256 : (h + 1) * 256].astype(BF16)
    await_bytes(tot_p, c_n - 1, tp_r)
    whole = jnp.sum(tot_p[...], axis=0)
    for q in range(4):
        tot_sum[q] = whole[q : q + 1, :]
    tot_z[my_z] = tot_sum[my_c // 2]

    to_protos(lambda peer: az_out.at[peer], az_in.at[my_z], az_s, az_r)
    to_protos(lambda peer: tot_z.at[my_z], tot_z.at[my_z], tz_s, tz_r)

    await_bytes(r2z, z_n - 1, r2z_r)
    column_pass(jnp.sum(r2z[...].astype(F32), axis=0))

    own_rows = pl.ds(pl.multiple_of(my_y * LANES, LANES), LANES)
    for k in range(COLS // CHUNK):
        cols = slice(k * CHUNK, (k + 1) * CHUNK)
        scaled = t[own_rows, cols] * v[0:1, cols]
        e[0:LANES, cols] = (scaled * s_scale[0:1, cols]).astype(BF16)
        halves = scaled[:, :LANES] + scaled[:, LANES:]
        part[0:LANES, :] = halves if k == 0 else part[0:LANES, :] + halves
    r3p[my_c] = lane_sums(part, 1)
    to_crops(lambda peer: r3p.at[my_c], r3p.at[my_c], r3p_s, r3p_r)
    sums = lax.dot_general(e[0:LANES, :], sp[...], NT, preferred_element_type=F32)
    for c in range(c_n):
        for g in range(2):
            ct_out[c, g] = sums[64 * g + 8 * c : 64 * g + 8 * c + 8, :].astype(BF16)
    to_crops(lambda peer: ct_out.at[peer], ct_in.at[my_c], ct_s, ct_r)
    ct_in[my_c] = ct_out[my_c]

    await_bytes(az_in, z_n - 1, az_r)
    az_in[my_z] = az_out[my_z]
    a_all[my_z] = jnp.sum(az_in[...].astype(F32), axis=0)
    to_protos(lambda peer: a_all.at[my_z], a_all.at[my_z], ag_s, ag_r)

    await_bytes(r3p, c_n - 1, r3p_r)
    r3z[my_z] = jnp.sum(r3p[...], axis=0)
    to_protos(lambda peer: r3z.at[my_z], r3z.at[my_z], r3z_s, r3z_r)
    await_bytes(ct_in, c_n - 1, ct_r)
    total = jnp.sum(ct_in[...].astype(F32), axis=0)
    mine = lax.rem(my_z, 4)
    for k in range(4):
        tile = total[:, :, k * LANES : (k + 1) * LANES].reshape(16, LANES)
        cz_out[k] = tile.astype(BF16)
    to_protos(lambda peer: cz_out.at[lax.rem(peer, 4)], cz_in.at[my_z], cz_s, cz_r)
    cz_in[my_z] = cz_out[mine]

    images = ROWS // c_n
    lane = lax.broadcasted_iota(jnp.int32, (images, LANES), 1)
    row = lax.broadcasted_iota(jnp.int32, (images, LANES), 0)

    def as_column(values, first, rows):
        n = values.shape[1]
        wide = jnp.broadcast_to(values, (rows, n))
        picked = jnp.where(lane[:rows, :n] == row[:rows, :n] + first, wide, jnp.zeros_like(wide))
        return jnp.sum(picked, axis=1, keepdims=True)

    loads[5].wait()
    weights = as_column(weight[...].astype(F32), 0, images)
    x = sf[...].astype(F32)
    unit = su[my_c].astype(F32)
    norm = lax.rsqrt(jnp.sum(x * x, axis=1, keepdims=True) + EPSILON)
    await_bytes(pairs, c_n - 1, pr_r)
    views = [as_column(pairs[c], my_c * 8, 8) > 0.5 for c in range(c_n)]
    await_bytes(tot_z, z_n - 1, tz_r)
    totals = as_column(jnp.sum(tot_z[...], axis=0), side * images, images)
    await_bytes(r3z, z_n - 1, r3z_r)
    last = 1.0 / jnp.sum(r3z[...], axis=0)
    scales = [as_column(last, images * g + my_c * 8, 8) for g in range(2)]

    await_bytes(cz_in, z_n - 1, cz_r)
    tile = jnp.sum(cz_in[...].astype(F32), axis=0)
    sides = [tile[8 * g : 8 * g + 8] * scales[g] for g in range(2)]
    for c in range(c_n):
        pick_out[c] = jnp.where(views[c], sides[1], sides[0])
    slot = mine * c_n + my_c

    def give_picks(k):
        step = lax.rem(k + 15, 4 * c_n - 1) + 1
        peer_c = lax.rem(my_c + lax.rem(step, c_n), c_n)
        pltpu.make_async_remote_copy(
            src_ref=pick_out.at[peer_c], dst_ref=pick_in.at[slot], send_sem=ca_s, recv_sem=ca_r,
            device_id={"crop": peer_c, "proto": lax.rem(my_z + z_n + 1 - lax.rem(step // c_n + 1, 4), z_n)},
            device_id_type=MESH,
        ).start()

    every(4 * c_n - 1, give_picks)
    pick_in[slot] = pick_out[my_c]
    await_bytes(a_all, z_n - 1, ag_r)
    for g in range(8):
        for h in range(2):
            rows = slice(g * 8, g * 8 + 8)
            grad_ref[rows, h * 256 : (h + 1) * 256] = a_all[2 * g + h] / totals[rows]
    await_bytes(pick_in, 4 * c_n - 1, ca_r)

    chosen = jnp.concatenate(
        [jnp.concatenate([pick_in[k * c_n + c] for k in range(4)], axis=1) for c in range(c_n)], axis=0
    )
    back = (weights * 10.0) * (grad_ref[...] - chosen)
    cross = jnp.sum(unit * chosen, axis=1, keepdims=True) * 10.0
    along = jnp.sum(x * back, axis=1, keepdims=True)
    grad_ref[...] = norm * back - norm * norm * norm * x * along
    losses = jnp.broadcast_to(jnp.log(totals) - cross, (images, images))
    eye = lane[:, :images] == row[:, :images]
    loss_ref[...] = jnp.sum(jnp.where(eye, losses, 0.0), axis=0, keepdims=True)

    for ref, n, sem in (
        (su, y_n - 1, tu_s), (su, y_n - 1, th_s), (col_sums, y_n - 1, cs_s),
        (su, c_n // 2 - 1, su_s), (su, c_n // 2, sh_s), (pairs, c_n - 1, pr_s),
        (r1p, y_n * c_n - 1, r1p_s), (r1z, z_n - 1, r1z_s),
        (r2p, c_n - 1, r2p_s), (r2z, z_n - 1, r2z_s), (tot_p, c_n - 1, tp_s),
        (tot_z, z_n - 1, tz_s), (a_in, c_n // 2 - 1, a_s),
        (az_in, z_n - 1, az_s), (a_all, z_n - 1, ag_s), (ct_in, c_n - 1, ct_s),
        (cz_in, z_n - 1, cz_s), (pick_in, 4 * c_n - 1, ca_s),
        (r3p, c_n - 1, r3p_s), (r3z, z_n - 1, r3z_s),
    ):
        await_bytes(ref, n, sem)
    pltpu.make_async_copy(a_mid, a_mid, am_s).wait()


def deliver(grad_in, loss_in, grad_ref, loss_ref):
    grad_ref[0] = grad_in[...]
    loss_ref[...] = loss_in[...]


def solution(mesh):
    y_n, c_n, z_n = (mesh.shape[a] for a in ("image", "crop", "proto"))

    def step(teacher_feats, student_feats, teacher_protos, student_protos, pairing, row_weight):
        images, views, width = teacher_feats.shape
        vmem = pl.BlockSpec(memory_space=pltpu.VMEM)
        hbm = pl.BlockSpec(memory_space=pltpu.HBM)
        dma = pltpu.SemaphoreType.DMA
        ram = pltpu.VMEM
        grad, loss = pl.pallas_call(
            functools.partial(kernel, y_n, c_n, z_n),
            out_shape=(
                jax.ShapeDtypeStruct((images, width), F32),
                jax.ShapeDtypeStruct((1, images), F32),
            ),
            in_specs=[hbm] * 6,
            out_specs=(vmem, vmem),
            scratch_shapes=[
                ram((images, views, width), BF16),
                ram((images, width), BF16),
                ram((1, images), jnp.int32),
                ram((1, images), BF16),
                ram((width, COLS), BF16),
                ram((width, COLS), BF16),
                ram((8, COLS), F32),
                ram((8, COLS), F32),
                ram((ROWS, COLS), F32),
                ram((ROWS, COLS), BF16),
                ram((y_n, views, images, width), BF16),
                ram((c_n, images, width), BF16),
                ram((ROWS, LANES), F32),
                ram((ROWS, LANES), F32),
                ram((ROWS, LANES), F32),
                ram((8, COLS), F32),
                ram((8, COLS), F32),
                ram((y_n * c_n, 1, LANES), F32),
                ram((z_n, 4, LANES), BF16),
                ram((c_n, 4, LANES), F32),
                ram((z_n, 4, LANES), BF16),
                ram((c_n, 4, LANES), F32),
                ram((4, 1, LANES), F32),
                ram((z_n, 1, LANES), F32),
                ram((c_n, 1, images), F32),
                ram((2, c_n // 2, images, width), BF16),
                ram((c_n // 2, images, width), BF16),
                ram((c_n // 2, images, width), BF16),
                ram((c_n // 2, images, width), BF16),
                ram((z_n, 8, 256), BF16),
                ram((z_n, 8, 256), BF16),
                ram((z_n, 8, 256), F32),
                ram((y_n, 1, COLS), F32),
                ram((c_n, 2, 8, width), BF16),
                ram((c_n, 2, 8, width), BF16),
                ram((4, 16, LANES), BF16),
                ram((z_n, 16, LANES), BF16),
                ram((c_n, 8, LANES), F32),
                ram((4 * c_n, 8, LANES), F32),
                ram((c_n, 1, LANES), F32),
                ram((z_n, 1, LANES), F32),
                dma((6,)),
                dma((y_n,)),
                dma((y_n,)),
            ]
            + [dma(())] * 40,
            compiler_params=pltpu.CompilerParams(
                collective_id=0, has_side_effects=True, vmem_limit_bytes=32 * 1024 * 1024
            ),
        )(
            *(
                pltpu.with_memory_space_constraint(x, pltpu.HBM)
                for x in (
                    teacher_feats,
                    student_feats.reshape(images, width),
                    pairing,
                    row_weight,
                    teacher_protos,
                    student_protos,
                )
            )
        )
        return pl.pallas_call(
            deliver,
            out_shape=(
                jax.ShapeDtypeStruct((1, images, width), F32),
                jax.ShapeDtypeStruct((1, images), F32),
            ),
            in_specs=[vmem] * 2,
            out_specs=(vmem, vmem),
            compiler_params=pltpu.CompilerParams(vmem_limit_bytes=2 * 1024 * 1024),
        )(grad, loss)

    return jax.shard_map(
        step,
        mesh=mesh,
        in_specs=(
            P("image", None, None),
            P("crop", "image", None),
            P(None, ("crop", "proto")),
            P(None, ("crop", "proto")),
            P("crop", "image"),
            P("crop", "image"),
        ),
        out_specs=(P("crop", "image", None), P("crop", "image")),
        check_vma=False,
    )
```

```python
import functools

import jax
import jax.numpy as jnp
from jax import lax
from jax.experimental import pallas as pl
from jax.experimental.pallas import tpu as pltpu
from jax.sharding import PartitionSpec as P

EPSILON = 1e-06
LOG2_E = 1.4426950408889634
TEACHER = 25.0 * LOG2_E
STUDENT = 10.0 * LOG2_E
MESH = pl.DeviceIdType.MESH
F32 = jnp.float32
BF16 = jnp.bfloat16
NT = (((1,), (1,)), ((), ()))
ROWS = 512
COLS = 2048
LANES = 128
CHUNK = 256


def every(n, body):
    lax.fori_loop(0, n, lambda k, c: (body(k), c)[1], 0)


def unit_rows(x):
    return x * lax.rsqrt(jnp.sum(x * x, axis=1, keepdims=True) + EPSILON)


def column_scales(raw, out):
    def chunk(j, carry):
        cols = pl.ds(pl.multiple_of(j * LANES, LANES), LANES)
        sums = jnp.zeros((8, LANES), F32)
        for r in range(8):
            w = raw[64 * r : 64 * r + 64, cols].astype(F32)
            sums = sums + jnp.sum((w * w).reshape(8, 8, LANES), axis=0)
        scale = lax.rsqrt(jnp.sum(sums, axis=0, keepdims=True) + EPSILON)
        out[:, cols] = jnp.broadcast_to(scale, (8, LANES))
        return carry

    lax.fori_loop(0, COLS // LANES, chunk, 0, unroll=4)


def lane_sums(ref, groups):
    sums = [
        jnp.sum(ref[q * LANES : (q + 1) * LANES, :].T, axis=0, keepdims=True) for q in range(groups)
    ]
    return jnp.concatenate(sums, axis=0) if groups > 1 else sums[0]


def kernel(
    y_n, c_n, z_n,
    tf_hbm, sf_hbm, pair_hbm, weight_hbm, tp_hbm, sp_hbm,
    grad_ref, loss_ref,
    tf, sf, pair, weight, tp, sp, t_scale, s_scale, t, e, tu, su, part, spart, ubuf, v, csum, acc,
    r1p, r1z, r2p, r2z, tot_p, tot_sum, tot_z, pairs,
    a_out, a_mid, a_pre, a_in, az_out, az_in, a_all, col_sums,
    ct_out, ct_in, cz_out, cz_in, pick_out, pick_in, r3p, r3z,
    load, tu_r, th_r,
    tu_s, th_s, su_s, su_r, sh_s, sh_r, pr_s, pr_r, r1p_s, r1p_r, r1z_s, r1z_r,
    r2p_s, r2p_r, r2z_s, r2z_r, tp_s, tp_r, tz_s, tz_r, a_s, a_r, az_s, az_r, ag_s, ag_r,
    am_s, am_r, cs_s, cs_r, ct_s, ct_r, cz_s, cz_r, ca_s, ca_r, r3p_s, r3p_r, r3z_s, r3z_r,
):
    my_y, my_c, my_z = (lax.axis_index(a) for a in ("image", "crop", "proto"))
    side = lax.rem(my_c, 2)
    partner = my_c + 1 - 2 * side

    loads = [
        pltpu.make_async_copy(src, dst, load.at[k])
        for k, (src, dst) in enumerate(
            ((tf_hbm, tf), (sf_hbm, sf), (tp_hbm, tp), (sp_hbm, sp), (pair_hbm, pair), (weight_hbm, weight))
        )
    ]

    def far_first(k):
        step = k + 1
        return z_n // 2 + (1 - 2 * lax.rem(step, 2)) * (step // 2)

    def push(src, dst, sends, recvs, axis, peer):
        pltpu.make_async_remote_copy(
            src_ref=src, dst_ref=dst, send_sem=sends, recv_sem=recvs,
            device_id={axis: peer}, device_id_type=MESH,
        ).start()

    def to_crops(src, dst, sends, recvs):
        def one(k):
            peer = lax.rem(my_c + lax.rem(k + 2, c_n - 1) + 1, c_n)
            push(src(peer), dst, sends, recvs, "crop", peer)

        every(c_n - 1, one)

    def to_protos(src, dst, sends, recvs):
        def one(k):
            peer = lax.rem(my_z + far_first(k), z_n)
            push(src(peer), dst, sends, recvs, "proto", peer)

        every(z_n - 1, one)

    def await_bytes(ref, n, sem):
        some = ref.at[pl.ds(0, n)]
        pltpu.make_async_copy(some, some, sem).wait()

    barrier = pltpu.get_barrier_semaphore()

    def greet(peer):
        pl.semaphore_signal(barrier, inc=1, device_id=peer, device_id_type=MESH)

    def plane_peer(k):
        step = lax.rem(k + 15, y_n * c_n - 1) + 1
        return {
            "image": lax.rem(my_y + step // c_n, y_n),
            "crop": lax.rem(my_c + lax.rem(step, c_n), c_n),
        }

    every(z_n - 1, lambda k: greet({"proto": lax.rem(my_z + far_first(k), z_n)}))
    for copy in loads:
        copy.start()
    every(y_n * c_n - 1, lambda k: greet(plane_peer(k)))

    loads[0].wait()
    for g in range(2):
        tu[my_y, g] = unit_rows(tf[:, g, :].astype(F32)).astype(BF16)
    loads[1].wait()
    su[my_c] = unit_rows(sf[...].astype(F32)).astype(BF16)
    loads[4].wait()
    pairs[my_c] = pair[...].astype(F32)
    loads[2].wait()
    column_scales(tp, t_scale)

    def transport(y, own):
        def chunk(i):
            for k in range(4):
                cols = pl.ds(pl.multiple_of((i * 4 + k) * CHUNK, CHUNK), CHUNK)
                rows = tu[y].reshape(LANES, ROWS)
                product = jnp.dot(rows, tp[:, cols], preferred_element_type=F32)
                terms = jnp.exp2(product * (t_scale[0:1, cols] * TEACHER))
                t[pl.ds(pl.multiple_of(y * LANES, LANES), LANES), cols] = terms
                if own:
                    csum[:, cols] = jnp.sum(terms.reshape(LANES // 8, 8, CHUNK), axis=0)

        every(2, chunk)

    transport(my_y, True)
    for k in range(COLS // LANES):
        cols = slice(k * LANES, (k + 1) * LANES)
        col_sums[my_y, :, cols] = jnp.sum(csum[:, cols], axis=0, keepdims=True)
    loads[3].wait()
    column_scales(sp, s_scale)

    pl.semaphore_wait(barrier, y_n * c_n + z_n - 2)

    def give_sums(k):
        peer = lax.rem(my_y + 2 - k + 3 * (k // 2), y_n)
        push(col_sums.at[my_y], col_sums.at[my_y], cs_s, cs_r, "image", peer)

    every(y_n - 1, give_sums)

    def give_rows(k):
        peer = lax.rem(my_y + 2 * k + 1 - 3 * (k // 2), y_n)
        push(tu.at[my_y, side], tu.at[my_y, side], tu_s, tu_r.at[my_y], "image", peer)

    every(y_n - 1, give_rows)

    def give_students(k):
        peer = lax.rem(my_c + 2 * k + 2, c_n)
        push(su.at[my_c], su.at[my_c], su_s, su_r, "crop", peer)

    every(c_n // 2 - 1, give_students)
    push(su.at[my_c], su.at[my_c], sh_s, sh_r, "crop", partner)
    to_crops(lambda peer: pairs.at[my_c], pairs.at[my_c], pr_s, pr_r)

    def hand_over(y):
        pltpu.make_async_copy(tu.at[y, side], tu.at[y, side], tu_r.at[y]).wait()
        push(tu.at[y, side], tu.at[y, side], th_s, th_r.at[y], "crop", partner)

    def handed(y):
        pltpu.make_async_copy(tu.at[y, side], tu.at[y, side], th_r.at[y]).wait()

    def set_v(sums):
        for k, s in enumerate(sums):
            v[:, k * LANES : (k + 1) * LANES] = jnp.broadcast_to(
                1.0 / jnp.sum(s, axis=0, keepdims=True), (8, LANES)
            )

    def row_pass(first, n):
        def block(r, carry):
            rows = pl.ds(pl.multiple_of(first + r * 8, 8), 8)
            total = t[rows, 0:LANES] * v[:, 0:LANES]
            for k in range(1, COLS // LANES):
                cols = slice(k * LANES, (k + 1) * LANES)
                total = total + t[rows, cols] * v[:, cols]
            part[pl.ds(pl.multiple_of(r * 8, 8), 8), :] = total
            return carry

        lax.fori_loop(0, n // 8, block, 0, unroll=4)
        return lane_sums(part, n // LANES)

    def column_pass(row_sums):
        u = 1.0 / row_sums
        for q in range(ROWS // LANES):
            ubuf[q * LANES : (q + 1) * LANES, :] = jnp.broadcast_to(u[q : q + 1, :], (LANES, LANES)).T

        def block(r, sums):
            rows = pl.ds(pl.multiple_of(r * 8, 8), 8)
            scale = ubuf[rows, :]
            return tuple(
                s + t[rows, k * LANES : (k + 1) * LANES] * scale for k, s in enumerate(sums)
            )

        zero = tuple(jnp.zeros((8, LANES), F32) for _ in range(COLS // LANES))
        set_v(lax.fori_loop(0, ROWS // 8, block, zero, unroll=4))

    await_bytes(col_sums, y_n - 1, cs_r)
    v[...] = jnp.broadcast_to(1.0 / jnp.sum(col_sums[...], axis=0), (8, COLS))
    mine_1 = my_y * c_n + my_c
    r1p[mine_1] = row_pass(my_y * LANES, LANES)

    def give_first(k):
        pltpu.make_async_remote_copy(
            src_ref=r1p.at[mine_1], dst_ref=r1p.at[mine_1], send_sem=r1p_s, recv_sem=r1p_r,
            device_id=plane_peer(k), device_id_type=MESH,
        ).start()

    every(y_n * c_n - 1, give_first)

    others = [lax.rem(my_y + k, y_n) for k in (1, 3, 2)]
    hand_over(others[0])
    hand_over(others[1])
    handed(others[0])
    transport(others[0], False)
    hand_over(others[2])
    await_bytes(su, c_n // 2 - 1, su_r)

    def hand_students(k):
        slot = lax.rem(my_c + 2 * k + 2, c_n)
        push(su.at[slot], su.at[slot], sh_s, sh_r, "crop", partner)

    every(c_n // 2 - 1, hand_students)
    handed(others[1])
    transport(others[1], False)
    handed(others[2])
    transport(others[2], False)

    await_bytes(r1p, y_n * c_n - 1, r1p_r)
    firsts = [jnp.sum(r1p[c_n * y : c_n * y + c_n], axis=0) for y in range(y_n)]
    r1z[my_z] = jnp.concatenate(firsts, axis=0).astype(BF16)
    to_protos(lambda peer: r1z.at[my_z], r1z.at[my_z], r1z_s, r1z_r)

    await_bytes(su, c_n // 2, sh_r)
    spart[...] = jnp.zeros_like(spart)

    def student(i):
        for k in range(2):
            cols = pl.ds(pl.multiple_of((2 * i + k) * CHUNK, CHUNK), CHUNK)
            for h in range(2):
                some = slice(256 * h, 256 * h + 256)
                rows = su[4 * h : 4 * h + 4].reshape(256, ROWS)
                product = jnp.dot(rows, sp[:, cols], preferred_element_type=F32)
                scale = s_scale[0:1, cols]
                terms = jnp.exp2(product * (scale * STUDENT))
                spart[some, :] += terms[:, :LANES] + terms[:, LANES:]
                e[some, cols] = (terms * scale).astype(BF16)

    every(COLS // CHUNK // 2, student)

    for j in range(2):
        some = slice(j * CHUNK, (j + 1) * CHUNK)
        acc[:, some] = lax.dot_general(e[...], sp[some, :], NT, preferred_element_type=F32)
    for c in range(c_n):
        rows = slice(64 * c, 64 * c + 64)
        unit = su[c].astype(F32)
        product = acc[rows, :] * unit
        shares = product[:, :LANES]
        for k in range(1, 4):
            shares = shares + product[:, k * LANES : (k + 1) * LANES]
        part[rows, :] = shares
        alpha = jnp.sum(shares, axis=1, keepdims=True)
        a_out[c % 2, c // 2] = (acc[rows, :] - alpha * unit).astype(BF16)
    push(a_out.at[1 - side], a_mid, am_s, am_r, "crop", partner)
    tot_p[my_c] = jnp.concatenate([lane_sums(spart, 4), lane_sums(part, 4)], axis=0)
    to_crops(lambda peer: tot_p.at[my_c], tot_p.at[my_c], tp_s, tp_r)
    pltpu.make_async_copy(a_mid, a_mid, am_r).wait()
    my_x = my_c // 2

    def merge(x):
        a_pre[x] = (a_out[side, x].astype(F32) + a_mid[x].astype(F32)).astype(BF16)

    every(c_n // 2, merge)

    def give_parts(k):
        x = lax.rem(my_x + k + 1, c_n // 2)
        push(a_pre.at[x], a_in.at[my_x], a_s, a_r, "crop", 2 * x + side)

    every(c_n // 2 - 1, give_parts)

    await_bytes(r1z, z_n - 1, r1z_r)
    column_pass(jnp.sum(r1z[...].astype(F32), axis=0))
    r2p[my_c] = row_pass(0, ROWS)
    to_crops(lambda peer: r2p.at[my_c], r2p.at[my_c], r2p_s, r2p_r)

    await_bytes(r2p, c_n - 1, r2p_r)
    r2z[my_z] = jnp.sum(r2p[...], axis=0).astype(BF16)
    to_protos(lambda peer: r2z.at[my_z], r2z.at[my_z], r2z_s, r2z_r)
    await_bytes(a_in, c_n // 2 - 1, a_r)
    a_in[my_x] = a_pre[my_x]
    for g in range(8):
        rows = slice(g * 8, g * 8 + 8)
        total = a_in[0, rows, :].astype(F32)
        for k in range(1, c_n // 2):
            total = total + a_in[k, rows, :].astype(F32)
        for h in range(2):
            az_out[2 * g + h] = total[:, h * 256 : (h + 1) * 256].astype(BF16)
    await_bytes(tot_p, c_n - 1, tp_r)
    whole = jnp.sum(tot_p[...], axis=0)
    for q in range(4):
        tot_sum[q] = jnp.concatenate([whole[q : q + 1, :], whole[q + 4 : q + 5, :]], axis=0)
    tot_z[my_z] = tot_sum[my_c // 2]

    to_protos(lambda peer: az_out.at[peer], az_in.at[my_z], az_s, az_r)
    to_protos(lambda peer: tot_z.at[my_z], tot_z.at[my_z], tz_s, tz_r)

    await_bytes(r2z, z_n - 1, r2z_r)
    column_pass(jnp.sum(r2z[...].astype(F32), axis=0))

    own_rows = pl.ds(pl.multiple_of(my_y * LANES, LANES), LANES)
    for k in range(COLS // CHUNK):
        cols = slice(k * CHUNK, (k + 1) * CHUNK)
        scaled = t[own_rows, cols] * v[0:1, cols]
        e[0:LANES, cols] = (scaled * s_scale[0:1, cols]).astype(BF16)
        halves = scaled[:, :LANES] + scaled[:, LANES:]
        part[0:LANES, :] = halves if k == 0 else part[0:LANES, :] + halves
    r3p[my_c] = lane_sums(part, 1)
    to_crops(lambda peer: r3p.at[my_c], r3p.at[my_c], r3p_s, r3p_r)
    sums = lax.dot_general(e[0:LANES, :], sp[...], NT, preferred_element_type=F32)
    for c in range(c_n):
        for g in range(2):
            ct_out[c, g] = sums[64 * g + 8 * c : 64 * g + 8 * c + 8, :].astype(BF16)
    to_crops(lambda peer: ct_out.at[peer], ct_in.at[my_c], ct_s, ct_r)
    ct_in[my_c] = ct_out[my_c]

    await_bytes(az_in, z_n - 1, az_r)
    az_in[my_z] = az_out[my_z]
    a_all[my_z] = jnp.sum(az_in[...].astype(F32), axis=0).astype(BF16)
    to_protos(lambda peer: a_all.at[my_z], a_all.at[my_z], ag_s, ag_r)

    await_bytes(r3p, c_n - 1, r3p_r)
    r3z[my_z] = jnp.sum(r3p[...], axis=0)
    to_protos(lambda peer: r3z.at[my_z], r3z.at[my_z], r3z_s, r3z_r)
    await_bytes(ct_in, c_n - 1, ct_r)
    total = jnp.sum(ct_in[...].astype(F32), axis=0)
    mine = lax.rem(my_z, 4)
    for k in range(4):
        tile = total[:, :, k * LANES : (k + 1) * LANES].reshape(16, LANES)
        cz_out[k] = tile.astype(BF16)
    to_protos(lambda peer: cz_out.at[lax.rem(peer, 4)], cz_in.at[my_z], cz_s, cz_r)
    cz_in[my_z] = cz_out[mine]

    images = ROWS // c_n
    lane = lax.broadcasted_iota(jnp.int32, (images, LANES), 1)
    row = lax.broadcasted_iota(jnp.int32, (images, LANES), 0)

    def as_column(values, first, rows):
        n = values.shape[1]
        wide = jnp.broadcast_to(values, (rows, n))
        picked = jnp.where(lane[:rows, :n] == row[:rows, :n] + first, wide, jnp.zeros_like(wide))
        return jnp.sum(picked, axis=1, keepdims=True)

    loads[5].wait()
    weights = as_column(weight[...].astype(F32), 0, images)
    x = sf[...].astype(F32)
    unit = su[my_c].astype(F32)
    norm = lax.rsqrt(jnp.sum(x * x, axis=1, keepdims=True) + EPSILON)
    await_bytes(pairs, c_n - 1, pr_r)
    views = [as_column(pairs[c], my_c * 8, 8) > 0.5 for c in range(c_n)]
    await_bytes(tot_z, z_n - 1, tz_r)
    both = jnp.sum(tot_z[...], axis=0)
    totals = as_column(both[0:1, :], side * images, images)
    alpha = as_column(both[1:2, :], side * images, images)
    await_bytes(r3z, z_n - 1, r3z_r)
    last = 1.0 / jnp.sum(r3z[...], axis=0)
    scales = [as_column(last, images * g + my_c * 8, 8) for g in range(2)]

    await_bytes(cz_in, z_n - 1, cz_r)
    tile = jnp.sum(cz_in[...].astype(F32), axis=0)
    sides = [tile[8 * g : 8 * g + 8] * scales[g] for g in range(2)]
    for c in range(c_n):
        pick_out[c] = jnp.where(views[c], sides[1], sides[0])
    slot = mine * c_n + my_c

    def give_picks(k):
        step = lax.rem(k + 15, 4 * c_n - 1) + 1
        peer_c = lax.rem(my_c + lax.rem(step, c_n), c_n)
        pltpu.make_async_remote_copy(
            src_ref=pick_out.at[peer_c], dst_ref=pick_in.at[slot], send_sem=ca_s, recv_sem=ca_r,
            device_id={"crop": peer_c, "proto": lax.rem(my_z + z_n + 1 - lax.rem(step // c_n + 1, 4), z_n)},
            device_id_type=MESH,
        ).start()

    every(4 * c_n - 1, give_picks)
    pick_in[slot] = pick_out[my_c]
    await_bytes(a_all, z_n - 1, ag_r)
    for g in range(8):
        for h in range(2):
            rows = slice(g * 8, g * 8 + 8)
            cols = slice(h * 256, (h + 1) * 256)
            whole = a_all[2 * g + h].astype(F32) + alpha[rows] * unit[rows, cols]
            grad_ref[rows, cols] = whole / totals[rows]
    await_bytes(pick_in, 4 * c_n - 1, ca_r)

    chosen = jnp.concatenate(
        [jnp.concatenate([pick_in[k * c_n + c] for k in range(4)], axis=1) for c in range(c_n)], axis=0
    )
    back = (weights * 10.0) * (grad_ref[...] - chosen)
    cross = jnp.sum(unit * chosen, axis=1, keepdims=True) * 10.0
    along = jnp.sum(x * back, axis=1, keepdims=True)
    grad_ref[...] = norm * back - norm * norm * norm * x * along
    losses = jnp.broadcast_to(jnp.log(totals) - cross, (images, images))
    eye = lane[:, :images] == row[:, :images]
    loss_ref[...] = jnp.sum(jnp.where(eye, losses, 0.0), axis=0, keepdims=True)

    for ref, n, sem in (
        (su, y_n - 1, tu_s), (su, y_n - 1, th_s), (col_sums, y_n - 1, cs_s),
        (su, c_n // 2 - 1, su_s), (su, c_n // 2, sh_s), (pairs, c_n - 1, pr_s),
        (r1p, y_n * c_n - 1, r1p_s), (r1z, z_n - 1, r1z_s),
        (r2p, c_n - 1, r2p_s), (r2z, z_n - 1, r2z_s), (tot_p, c_n - 1, tp_s),
        (tot_z, z_n - 1, tz_s), (a_in, c_n // 2 - 1, a_s),
        (az_in, z_n - 1, az_s), (a_all, z_n - 1, ag_s), (ct_in, c_n - 1, ct_s),
        (cz_in, z_n - 1, cz_s), (pick_in, 4 * c_n - 1, ca_s),
        (r3p, c_n - 1, r3p_s), (r3z, z_n - 1, r3z_s),
    ):
        await_bytes(ref, n, sem)
    pltpu.make_async_copy(a_mid, a_mid, am_s).wait()


def deliver(grad_in, loss_in, grad_ref, loss_ref):
    grad_ref[0] = grad_in[...]
    loss_ref[...] = loss_in[...]


def solution(mesh):
    y_n, c_n, z_n = (mesh.shape[a] for a in ("image", "crop", "proto"))

    def step(teacher_feats, student_feats, teacher_protos, student_protos, pairing, row_weight):
        images, views, width = teacher_feats.shape
        vmem = pl.BlockSpec(memory_space=pltpu.VMEM)
        hbm = pl.BlockSpec(memory_space=pltpu.HBM)
        dma = pltpu.SemaphoreType.DMA
        ram = pltpu.VMEM
        grad, loss = pl.pallas_call(
            functools.partial(kernel, y_n, c_n, z_n),
            out_shape=(
                jax.ShapeDtypeStruct((images, width), F32),
                jax.ShapeDtypeStruct((1, images), F32),
            ),
            in_specs=[hbm] * 6,
            out_specs=(vmem, vmem),
            scratch_shapes=[
                ram((images, views, width), BF16),
                ram((images, width), BF16),
                ram((1, images), jnp.int32),
                ram((1, images), BF16),
                ram((width, COLS), BF16),
                ram((width, COLS), BF16),
                ram((8, COLS), F32),
                ram((8, COLS), F32),
                ram((ROWS, COLS), F32),
                ram((ROWS, COLS), BF16),
                ram((y_n, views, images, width), BF16),
                ram((c_n, images, width), BF16),
                ram((ROWS, LANES), F32),
                ram((ROWS, LANES), F32),
                ram((ROWS, LANES), F32),
                ram((8, COLS), F32),
                ram((8, COLS), F32),
                ram((ROWS, ROWS), F32),
                ram((y_n * c_n, 1, LANES), F32),
                ram((z_n, 4, LANES), BF16),
                ram((c_n, 4, LANES), F32),
                ram((z_n, 4, LANES), BF16),
                ram((c_n, 8, LANES), F32),
                ram((4, 2, LANES), F32),
                ram((z_n, 2, LANES), F32),
                ram((c_n, 1, images), F32),
                ram((2, c_n // 2, images, width), BF16),
                ram((c_n // 2, images, width), BF16),
                ram((c_n // 2, images, width), BF16),
                ram((c_n // 2, images, width), BF16),
                ram((z_n, 8, 256), BF16),
                ram((z_n, 8, 256), BF16),
                ram((z_n, 8, 256), BF16),
                ram((y_n, 1, COLS), F32),
                ram((c_n, 2, 8, width), BF16),
                ram((c_n, 2, 8, width), BF16),
                ram((4, 16, LANES), BF16),
                ram((z_n, 16, LANES), BF16),
                ram((c_n, 8, LANES), F32),
                ram((4 * c_n, 8, LANES), F32),
                ram((c_n, 1, LANES), F32),
                ram((z_n, 1, LANES), F32),
                dma((6,)),
                dma((y_n,)),
                dma((y_n,)),
            ]
            + [dma(())] * 40,
            compiler_params=pltpu.CompilerParams(
                collective_id=0, has_side_effects=True, vmem_limit_bytes=32 * 1024 * 1024
            ),
        )(
            *(
                pltpu.with_memory_space_constraint(x, pltpu.HBM)
                for x in (
                    teacher_feats,
                    student_feats.reshape(images, width),
                    pairing,
                    row_weight,
                    teacher_protos,
                    student_protos,
                )
            )
        )
        return pl.pallas_call(
            deliver,
            out_shape=(
                jax.ShapeDtypeStruct((1, images, width), F32),
                jax.ShapeDtypeStruct((1, images), F32),
            ),
            in_specs=[vmem] * 2,
            out_specs=(vmem, vmem),
            compiler_params=pltpu.CompilerParams(vmem_limit_bytes=2 * 1024 * 1024),
        )(grad, loss)

    return jax.shard_map(
        step,
        mesh=mesh,
        in_specs=(
            P("image", None, None),
            P("crop", "image", None),
            P(None, ("crop", "proto")),
            P(None, ("crop", "proto")),
            P("crop", "image"),
            P("crop", "image"),
        ),
        out_specs=(P("crop", "image", None), P("crop", "image")),
        check_vma=False,
    )
```

```python
import functools

import jax
import jax.numpy as jnp
from jax import lax
from jax.experimental import pallas as pl
from jax.experimental.pallas import tpu as pltpu
from jax.sharding import PartitionSpec as P

EPSILON = 1e-06
LOG2_E = 1.4426950408889634
TEACHER = 25.0 * LOG2_E
STUDENT = 10.0 * LOG2_E
MESH = pl.DeviceIdType.MESH
F32 = jnp.float32
BF16 = jnp.bfloat16
NT = (((1,), (1,)), ((), ()))
ROWS = 512
COLS = 2048
LANES = 128
CHUNK = 256


def every(n, body):
    lax.fori_loop(0, n, lambda k, c: (body(k), c)[1], 0)


def unit_rows(x):
    return x * lax.rsqrt(jnp.sum(x * x, axis=1, keepdims=True) + EPSILON)


def column_scales(raw, out):
    def chunk(j, carry):
        cols = pl.ds(pl.multiple_of(j * LANES, LANES), LANES)
        sums = jnp.zeros((8, LANES), F32)
        for r in range(8):
            w = raw[64 * r : 64 * r + 64, cols].astype(F32)
            sums = sums + jnp.sum((w * w).reshape(8, 8, LANES), axis=0)
        scale = lax.rsqrt(jnp.sum(sums, axis=0, keepdims=True) + EPSILON)
        out[:, cols] = jnp.broadcast_to(scale, (8, LANES))
        return carry

    lax.fori_loop(0, COLS // LANES, chunk, 0, unroll=4)


def lane_sums(ref, groups):
    sums = [
        jnp.sum(ref[q * LANES : (q + 1) * LANES, :].T, axis=0, keepdims=True) for q in range(groups)
    ]
    return jnp.concatenate(sums, axis=0) if groups > 1 else sums[0]


def kernel(
    y_n, c_n, z_n,
    tf_hbm, sf_hbm, pair_hbm, weight_hbm, tp_hbm, sp_hbm,
    grad_ref, loss_ref,
    tf, sf, pair, weight, tp, sp, t_scale, s_scale, t, e, tu, su, part, spart, ubuf, v, csum, acc,
    r1p, r1z, r2p, r2z, tot_p, tot_sum, tot_z, pairs,
    a_out, a_mid, a_pre, a_in, az_out, az_in, a_all, col_sums,
    ct_out, ct_in, cz_out, cz_in, pick_out, pick_in, r3p, r3z,
    load, tu_r, th_r,
    tu_s, th_s, su_s, su_r, sh_s, sh_r, pr_s, pr_r, r1p_s, r1p_r, r1z_s, r1z_r,
    r2p_s, r2p_r, r2z_s, r2z_r, tp_s, tp_r, tz_s, tz_r, a_s, a_r, az_s, az_r, ag_s, ag_r,
    am_s, am_r, cs_s, cs_r, ct_s, ct_r, cz_s, cz_r, ca_s, ca_r, r3p_s, r3p_r, r3z_s, r3z_r,
):
    my_y, my_c, my_z = (lax.axis_index(a) for a in ("image", "crop", "proto"))
    side = lax.rem(my_c, 2)
    partner = my_c + 1 - 2 * side

    loads = [
        pltpu.make_async_copy(src, dst, load.at[k])
        for k, (src, dst) in enumerate(
            ((tf_hbm, tf), (sf_hbm, sf), (tp_hbm, tp), (sp_hbm, sp), (pair_hbm, pair), (weight_hbm, weight))
        )
    ]

    def far_first(k):
        step = k + 1
        return z_n // 2 + (1 - 2 * lax.rem(step, 2)) * (step // 2)

    def push(src, dst, sends, recvs, axis, peer):
        pltpu.make_async_remote_copy(
            src_ref=src, dst_ref=dst, send_sem=sends, recv_sem=recvs,
            device_id={axis: peer}, device_id_type=MESH,
        ).start()

    def to_crops(src, dst, sends, recvs):
        def one(k):
            peer = lax.rem(my_c + lax.rem(k + 2, c_n - 1) + 1, c_n)
            push(src(peer), dst, sends, recvs, "crop", peer)

        every(c_n - 1, one)

    def to_protos(src, dst, sends, recvs):
        def one(k):
            peer = lax.rem(my_z + far_first(k), z_n)
            push(src(peer), dst, sends, recvs, "proto", peer)

        every(z_n - 1, one)

    def await_bytes(ref, n, sem):
        some = ref.at[pl.ds(0, n)]
        pltpu.make_async_copy(some, some, sem).wait()

    barrier = pltpu.get_barrier_semaphore()

    def greet(peer):
        pl.semaphore_signal(barrier, inc=1, device_id=peer, device_id_type=MESH)

    def plane_peer(k):
        step = lax.rem(k + 15, y_n * c_n - 1) + 1
        return {
            "image": lax.rem(my_y + step // c_n, y_n),
            "crop": lax.rem(my_c + lax.rem(step, c_n), c_n),
        }

    every(z_n - 1, lambda k: greet({"proto": lax.rem(my_z + far_first(k), z_n)}))
    for copy in loads:
        copy.start()
    every(y_n * c_n - 1, lambda k: greet(plane_peer(k)))

    loads[0].wait()
    for g in range(2):
        tu[my_y, g] = unit_rows(tf[:, g, :].astype(F32)).astype(BF16)
    loads[1].wait()
    su[my_c] = unit_rows(sf[...].astype(F32)).astype(BF16)
    loads[4].wait()
    pairs[my_c] = pair[...].astype(F32)
    loads[2].wait()
    column_scales(tp, t_scale)

    def transport(y, own):
        def chunk(i):
            for k in range(4):
                cols = pl.ds(pl.multiple_of((i * 4 + k) * CHUNK, CHUNK), CHUNK)
                rows = tu[y].reshape(LANES, ROWS)
                product = jnp.dot(rows, tp[:, cols], preferred_element_type=F32)
                terms = jnp.exp2(product * (t_scale[0:1, cols] * TEACHER))
                t[pl.ds(pl.multiple_of(y * LANES, LANES), LANES), cols] = terms
                if own:
                    csum[:, cols] = jnp.sum(terms.reshape(LANES // 8, 8, CHUNK), axis=0)

        every(2, chunk)

    transport(my_y, True)
    for k in range(COLS // LANES):
        cols = slice(k * LANES, (k + 1) * LANES)
        col_sums[my_y, :, cols] = jnp.sum(csum[:, cols], axis=0, keepdims=True)
    loads[3].wait()
    column_scales(sp, s_scale)

    pl.semaphore_wait(barrier, y_n * c_n + z_n - 2)

    def give_sums(k):
        peer = lax.rem(my_y + 2 - k + 3 * (k // 2), y_n)
        push(col_sums.at[my_y], col_sums.at[my_y], cs_s, cs_r, "image", peer)

    every(y_n - 1, give_sums)

    def give_rows(k):
        peer = lax.rem(my_y + 2 * k + 1 - 3 * (k // 2), y_n)
        push(tu.at[my_y, side], tu.at[my_y, side], tu_s, tu_r.at[my_y], "image", peer)

    every(y_n - 1, give_rows)

    def give_students(k):
        peer = lax.rem(my_c + 2 * k + 2, c_n)
        push(su.at[my_c], su.at[my_c], su_s, su_r, "crop", peer)

    every(c_n // 2 - 1, give_students)
    push(su.at[my_c], su.at[my_c], sh_s, sh_r, "crop", partner)
    to_crops(lambda peer: pairs.at[my_c], pairs.at[my_c], pr_s, pr_r)

    def hand_over(y):
        pltpu.make_async_copy(tu.at[y, side], tu.at[y, side], tu_r.at[y]).wait()
        push(tu.at[y, side], tu.at[y, side], th_s, th_r.at[y], "crop", partner)

    def handed(y):
        pltpu.make_async_copy(tu.at[y, side], tu.at[y, side], th_r.at[y]).wait()

    def set_v(sums):
        for k, s in enumerate(sums):
            v[:, k * LANES : (k + 1) * LANES] = jnp.broadcast_to(
                1.0 / jnp.sum(s, axis=0, keepdims=True), (8, LANES)
            )

    def row_pass(first, n):
        def block(r, carry):
            rows = pl.ds(pl.multiple_of(first + r * 8, 8), 8)
            total = t[rows, 0:LANES] * v[:, 0:LANES]
            for k in range(1, COLS // LANES):
                cols = slice(k * LANES, (k + 1) * LANES)
                total = total + t[rows, cols] * v[:, cols]
            part[pl.ds(pl.multiple_of(r * 8, 8), 8), :] = total
            return carry

        lax.fori_loop(0, n // 8, block, 0, unroll=8)
        return lane_sums(part, n // LANES)

    def column_pass(row_sums):
        u = 1.0 / row_sums
        for q in range(ROWS // LANES):
            ubuf[q * LANES : (q + 1) * LANES, :] = jnp.broadcast_to(u[q : q + 1, :], (LANES, LANES)).T

        def block(r, sums):
            rows = pl.ds(pl.multiple_of(r * 8, 8), 8)
            scale = ubuf[rows, :]
            return tuple(
                s + t[rows, k * LANES : (k + 1) * LANES] * scale for k, s in enumerate(sums)
            )

        zero = tuple(jnp.zeros((8, LANES), F32) for _ in range(COLS // LANES))
        set_v(lax.fori_loop(0, ROWS // 8, block, zero, unroll=8))

    await_bytes(col_sums, y_n - 1, cs_r)
    v[...] = jnp.broadcast_to(1.0 / jnp.sum(col_sums[...], axis=0), (8, COLS))
    mine_1 = my_y * c_n + my_c
    r1p[mine_1] = row_pass(my_y * LANES, LANES)

    def give_first(k):
        pltpu.make_async_remote_copy(
            src_ref=r1p.at[mine_1], dst_ref=r1p.at[mine_1], send_sem=r1p_s, recv_sem=r1p_r,
            device_id=plane_peer(k), device_id_type=MESH,
        ).start()

    every(y_n * c_n - 1, give_first)

    others = [lax.rem(my_y + k, y_n) for k in (1, 3, 2)]
    hand_over(others[0])
    hand_over(others[1])
    handed(others[0])
    transport(others[0], False)
    hand_over(others[2])
    await_bytes(su, c_n // 2 - 1, su_r)

    def hand_students(k):
        slot = lax.rem(my_c + 2 * k + 2, c_n)
        push(su.at[slot], su.at[slot], sh_s, sh_r, "crop", partner)

    every(c_n // 2 - 1, hand_students)
    handed(others[1])
    transport(others[1], False)
    handed(others[2])
    transport(others[2], False)

    await_bytes(r1p, y_n * c_n - 1, r1p_r)
    firsts = [jnp.sum(r1p[c_n * y : c_n * y + c_n], axis=0) for y in range(y_n)]
    r1z[my_z] = jnp.concatenate(firsts, axis=0).astype(BF16)
    to_protos(lambda peer: r1z.at[my_z], r1z.at[my_z], r1z_s, r1z_r)

    await_bytes(su, c_n // 2, sh_r)
    spart[...] = jnp.zeros_like(spart)

    def student(i):
        for k in range(2):
            cols = pl.ds(pl.multiple_of((2 * i + k) * CHUNK, CHUNK), CHUNK)
            for h in range(2):
                some = slice(256 * h, 256 * h + 256)
                rows = su[4 * h : 4 * h + 4].reshape(256, ROWS)
                product = jnp.dot(rows, sp[:, cols], preferred_element_type=F32)
                scale = s_scale[0:1, cols]
                terms = jnp.exp2(product * (scale * STUDENT))
                spart[some, :] += terms[:, :LANES] + terms[:, LANES:]
                e[some, cols] = (terms * scale).astype(BF16)

    every(COLS // CHUNK // 2, student)

    for j in range(2):
        some = slice(j * CHUNK, (j + 1) * CHUNK)
        acc[:, some] = lax.dot_general(e[...], sp[some, :], NT, preferred_element_type=F32)
    for c in range(c_n):
        rows = slice(64 * c, 64 * c + 64)
        unit = su[c].astype(F32)
        product = acc[rows, :] * unit
        shares = product[:, :LANES]
        for k in range(1, 4):
            shares = shares + product[:, k * LANES : (k + 1) * LANES]
        part[rows, :] = shares
        alpha = jnp.sum(shares, axis=1, keepdims=True)
        rest = acc[rows, :] - alpha * unit
        acc[rows, :] = rest
        a_out[c % 2, c // 2] = rest.astype(BF16)
    push(a_out.at[1 - side], a_mid, am_s, am_r, "crop", partner)
    tot_p[my_c] = jnp.concatenate([lane_sums(spart, 4), lane_sums(part, 4)], axis=0)
    to_crops(lambda peer: tot_p.at[my_c], tot_p.at[my_c], tp_s, tp_r)
    pltpu.make_async_copy(a_mid, a_mid, am_r).wait()
    my_x = my_c // 2

    def merge(x):
        rows = pl.ds(pl.multiple_of((2 * x + side) * 64, 64), 64)
        a_pre[x] = (acc[rows, :] + a_mid[x].astype(F32)).astype(BF16)

    every(c_n // 2, merge)

    def give_parts(k):
        x = lax.rem(my_x + k + 1, c_n // 2)
        push(a_pre.at[x], a_in.at[my_x], a_s, a_r, "crop", 2 * x + side)

    every(c_n // 2 - 1, give_parts)

    await_bytes(r1z, z_n - 1, r1z_r)
    column_pass(jnp.sum(r1z[...].astype(F32), axis=0))
    r2p[my_c] = row_pass(0, ROWS)
    to_crops(lambda peer: r2p.at[my_c], r2p.at[my_c], r2p_s, r2p_r)

    await_bytes(r2p, c_n - 1, r2p_r)
    r2z[my_z] = jnp.sum(r2p[...], axis=0).astype(BF16)
    to_protos(lambda peer: r2z.at[my_z], r2z.at[my_z], r2z_s, r2z_r)
    await_bytes(a_in, c_n // 2 - 1, a_r)
    a_in[my_x] = a_pre[my_x]
    for g in range(8):
        rows = slice(g * 8, g * 8 + 8)
        total = a_in[0, rows, :].astype(F32)
        for k in range(1, c_n // 2):
            total = total + a_in[k, rows, :].astype(F32)
        for h in range(2):
            az_out[2 * g + h] = total[:, h * 256 : (h + 1) * 256].astype(BF16)
    await_bytes(tot_p, c_n - 1, tp_r)
    whole = jnp.sum(tot_p[...], axis=0)
    for q in range(4):
        tot_sum[q] = jnp.concatenate([whole[q : q + 1, :], whole[q + 4 : q + 5, :]], axis=0)
    tot_z[my_z] = tot_sum[my_c // 2]

    to_protos(lambda peer: az_out.at[peer], az_in.at[my_z], az_s, az_r)
    to_protos(lambda peer: tot_z.at[my_z], tot_z.at[my_z], tz_s, tz_r)

    await_bytes(r2z, z_n - 1, r2z_r)
    column_pass(jnp.sum(r2z[...].astype(F32), axis=0))

    own_rows = pl.ds(pl.multiple_of(my_y * LANES, LANES), LANES)
    for k in range(COLS // CHUNK):
        cols = slice(k * CHUNK, (k + 1) * CHUNK)
        scaled = t[own_rows, cols] * v[0:1, cols]
        e[0:LANES, cols] = (scaled * s_scale[0:1, cols]).astype(BF16)
        halves = scaled[:, :LANES] + scaled[:, LANES:]
        part[0:LANES, :] = halves if k == 0 else part[0:LANES, :] + halves
    sums = lax.dot_general(e[0:LANES, :], sp[...], NT, preferred_element_type=F32)
    for c in range(c_n):
        for g in range(2):
            ct_out[c, g] = sums[64 * g + 8 * c : 64 * g + 8 * c + 8, :].astype(BF16)
    to_crops(lambda peer: ct_out.at[peer], ct_in.at[my_c], ct_s, ct_r)
    r3p[my_c] = lane_sums(part, 1)
    to_crops(lambda peer: r3p.at[my_c], r3p.at[my_c], r3p_s, r3p_r)
    ct_in[my_c] = ct_out[my_c]

    await_bytes(az_in, z_n - 1, az_r)
    az_in[my_z] = az_out[my_z]
    a_all[my_z] = jnp.sum(az_in[...].astype(F32), axis=0).astype(BF16)
    to_protos(lambda peer: a_all.at[my_z], a_all.at[my_z], ag_s, ag_r)

    await_bytes(ct_in, c_n - 1, ct_r)
    total = jnp.sum(ct_in[...].astype(F32), axis=0)
    mine = lax.rem(my_z, 4)
    for k in range(4):
        tile = total[:, :, k * LANES : (k + 1) * LANES].reshape(16, LANES)
        cz_out[k] = tile.astype(BF16)
    to_protos(lambda peer: cz_out.at[lax.rem(peer, 4)], cz_in.at[my_z], cz_s, cz_r)
    await_bytes(r3p, c_n - 1, r3p_r)
    r3z[my_z] = jnp.sum(r3p[...], axis=0)
    to_protos(lambda peer: r3z.at[my_z], r3z.at[my_z], r3z_s, r3z_r)
    cz_in[my_z] = cz_out[mine]

    images = ROWS // c_n
    lane = lax.broadcasted_iota(jnp.int32, (images, LANES), 1)
    row = lax.broadcasted_iota(jnp.int32, (images, LANES), 0)

    def as_column(values, first, rows):
        n = values.shape[1]
        wide = jnp.broadcast_to(values, (rows, n))
        picked = jnp.where(lane[:rows, :n] == row[:rows, :n] + first, wide, jnp.zeros_like(wide))
        return jnp.sum(picked, axis=1, keepdims=True)

    loads[5].wait()
    weights = as_column(weight[...].astype(F32), 0, images)
    x = sf[...].astype(F32)
    unit = su[my_c].astype(F32)
    norm = lax.rsqrt(jnp.sum(x * x, axis=1, keepdims=True) + EPSILON)
    await_bytes(pairs, c_n - 1, pr_r)
    views = [as_column(pairs[c], my_c * 8, 8) > 0.5 for c in range(c_n)]
    await_bytes(tot_z, z_n - 1, tz_r)
    both = jnp.sum(tot_z[...], axis=0)
    totals = as_column(both[0:1, :], side * images, images)
    alpha = as_column(both[1:2, :], side * images, images)
    await_bytes(r3z, z_n - 1, r3z_r)
    last = 1.0 / jnp.sum(r3z[...], axis=0)
    scales = [as_column(last, images * g + my_c * 8, 8) for g in range(2)]

    await_bytes(cz_in, z_n - 1, cz_r)
    tile = jnp.sum(cz_in[...].astype(F32), axis=0)
    sides = [tile[8 * g : 8 * g + 8] * scales[g] for g in range(2)]
    for c in range(c_n):
        pick_out[c] = jnp.where(views[c], sides[1], sides[0])
    slot = mine * c_n + my_c

    def give_picks(k):
        step = lax.rem(k + 15, 4 * c_n - 1) + 1
        peer_c = lax.rem(my_c + lax.rem(step, c_n), c_n)
        pltpu.make_async_remote_copy(
            src_ref=pick_out.at[peer_c], dst_ref=pick_in.at[slot], send_sem=ca_s, recv_sem=ca_r,
            device_id={"crop": peer_c, "proto": lax.rem(my_z + z_n + 1 - lax.rem(step // c_n + 1, 4), z_n)},
            device_id_type=MESH,
        ).start()

    every(4 * c_n - 1, give_picks)
    pick_in[slot] = pick_out[my_c]
    await_bytes(a_all, z_n - 1, ag_r)
    for g in range(8):
        for h in range(2):
            rows = slice(g * 8, g * 8 + 8)
            cols = slice(h * 256, (h + 1) * 256)
            whole = a_all[2 * g + h].astype(F32) + alpha[rows] * unit[rows, cols]
            grad_ref[rows, cols] = whole / totals[rows]
    await_bytes(pick_in, 4 * c_n - 1, ca_r)

    chosen = jnp.concatenate(
        [jnp.concatenate([pick_in[k * c_n + c] for k in range(4)], axis=1) for c in range(c_n)], axis=0
    )
    back = (weights * 10.0) * (grad_ref[...] - chosen)
    cross = jnp.sum(unit * chosen, axis=1, keepdims=True) * 10.0
    along = jnp.sum(x * back, axis=1, keepdims=True)
    grad_ref[...] = norm * back - norm * norm * norm * x * along
    losses = jnp.broadcast_to(jnp.log(totals) - cross, (images, images))
    eye = lane[:, :images] == row[:, :images]
    loss_ref[...] = jnp.sum(jnp.where(eye, losses, 0.0), axis=0, keepdims=True)

    for ref, n, sem in (
        (su, y_n - 1, tu_s), (su, y_n - 1, th_s), (col_sums, y_n - 1, cs_s),
        (su, c_n // 2 - 1, su_s), (su, c_n // 2, sh_s), (pairs, c_n - 1, pr_s),
        (r1p, y_n * c_n - 1, r1p_s), (r1z, z_n - 1, r1z_s),
        (r2p, c_n - 1, r2p_s), (r2z, z_n - 1, r2z_s), (tot_p, c_n - 1, tp_s),
        (tot_z, z_n - 1, tz_s), (a_in, c_n // 2 - 1, a_s),
        (az_in, z_n - 1, az_s), (a_all, z_n - 1, ag_s), (ct_in, c_n - 1, ct_s),
        (cz_in, z_n - 1, cz_s), (pick_in, 4 * c_n - 1, ca_s),
        (r3p, c_n - 1, r3p_s), (r3z, z_n - 1, r3z_s),
    ):
        await_bytes(ref, n, sem)
    pltpu.make_async_copy(a_mid, a_mid, am_s).wait()


def deliver(grad_in, loss_in, grad_ref, loss_ref):
    grad_ref[0] = grad_in[...]
    loss_ref[...] = loss_in[...]


def solution(mesh):
    y_n, c_n, z_n = (mesh.shape[a] for a in ("image", "crop", "proto"))

    def step(teacher_feats, student_feats, teacher_protos, student_protos, pairing, row_weight):
        images, views, width = teacher_feats.shape
        vmem = pl.BlockSpec(memory_space=pltpu.VMEM)
        hbm = pl.BlockSpec(memory_space=pltpu.HBM)
        dma = pltpu.SemaphoreType.DMA
        ram = pltpu.VMEM
        grad, loss = pl.pallas_call(
            functools.partial(kernel, y_n, c_n, z_n),
            out_shape=(
                jax.ShapeDtypeStruct((images, width), F32),
                jax.ShapeDtypeStruct((1, images), F32),
            ),
            in_specs=[hbm] * 6,
            out_specs=(vmem, vmem),
            scratch_shapes=[
                ram((images, views, width), BF16),
                ram((images, width), BF16),
                ram((1, images), jnp.int32),
                ram((1, images), BF16),
                ram((width, COLS), BF16),
                ram((width, COLS), BF16),
                ram((8, COLS), F32),
                ram((8, COLS), F32),
                ram((ROWS, COLS), F32),
                ram((ROWS, COLS), BF16),
                ram((y_n, views, images, width), BF16),
                ram((c_n, images, width), BF16),
                ram((ROWS, LANES), F32),
                ram((ROWS, LANES), F32),
                ram((ROWS, LANES), F32),
                ram((8, COLS), F32),
                ram((8, COLS), F32),
                ram((ROWS, ROWS), F32),
                ram((y_n * c_n, 1, LANES), F32),
                ram((z_n, 4, LANES), BF16),
                ram((c_n, 4, LANES), F32),
                ram((z_n, 4, LANES), BF16),
                ram((c_n, 8, LANES), F32),
                ram((4, 2, LANES), F32),
                ram((z_n, 2, LANES), F32),
                ram((c_n, 1, images), F32),
                ram((2, c_n // 2, images, width), BF16),
                ram((c_n // 2, images, width), BF16),
                ram((c_n // 2, images, width), BF16),
                ram((c_n // 2, images, width), BF16),
                ram((z_n, 8, 256), BF16),
                ram((z_n, 8, 256), BF16),
                ram((z_n, 8, 256), BF16),
                ram((y_n, 1, COLS), F32),
                ram((c_n, 2, 8, width), BF16),
                ram((c_n, 2, 8, width), BF16),
                ram((4, 16, LANES), BF16),
                ram((z_n, 16, LANES), BF16),
                ram((c_n, 8, LANES), F32),
                ram((4 * c_n, 8, LANES), F32),
                ram((c_n, 1, LANES), F32),
                ram((z_n, 1, LANES), F32),
                dma((6,)),
                dma((y_n,)),
                dma((y_n,)),
            ]
            + [dma(())] * 40,
            compiler_params=pltpu.CompilerParams(
                collective_id=0, has_side_effects=True, vmem_limit_bytes=32 * 1024 * 1024
            ),
        )(
            *(
                pltpu.with_memory_space_constraint(x, pltpu.HBM)
                for x in (
                    teacher_feats,
                    student_feats.reshape(images, width),
                    pairing,
                    row_weight,
                    teacher_protos,
                    student_protos,
                )
            )
        )
        return pl.pallas_call(
            deliver,
            out_shape=(
                jax.ShapeDtypeStruct((1, images, width), F32),
                jax.ShapeDtypeStruct((1, images), F32),
            ),
            in_specs=[vmem] * 2,
            out_specs=(vmem, vmem),
            compiler_params=pltpu.CompilerParams(vmem_limit_bytes=2 * 1024 * 1024),
        )(grad, loss)

    return jax.shard_map(
        step,
        mesh=mesh,
        in_specs=(
            P("image", None, None),
            P("crop", "image", None),
            P(None, ("crop", "proto")),
            P(None, ("crop", "proto")),
            P("crop", "image"),
            P("crop", "image"),
        ),
        out_specs=(P("crop", "image", None), P("crop", "image")),
        check_vma=False,
    )
```

```python
import functools

import jax
import jax.numpy as jnp
from jax import lax
from jax.experimental import pallas as pl
from jax.experimental.pallas import tpu as pltpu
from jax.sharding import PartitionSpec as P

EPSILON = 1e-06
LOG2_E = 1.4426950408889634
TEACHER = 25.0 * LOG2_E
STUDENT = 10.0 * LOG2_E
MESH = pl.DeviceIdType.MESH
F32 = jnp.float32
BF16 = jnp.bfloat16
NT = (((1,), (1,)), ((), ()))
ROWS = 512
COLS = 2048
LANES = 128
CHUNK = 256


def every(n, body):
    unroll = next(u for u in (31, 7, 5, 3, 1) if n % u == 0) if n > 2 else 1
    lax.fori_loop(0, n, lambda k, c: (body(k), c)[1], 0, unroll=unroll)


def unit_rows(x):
    return x * lax.rsqrt(jnp.sum(x * x, axis=1, keepdims=True) + EPSILON)


def column_scales(raw, out):
    def chunk(j, carry):
        cols = pl.ds(pl.multiple_of(j * LANES, LANES), LANES)
        sums = jnp.zeros((8, LANES), F32)
        for r in range(8):
            w = raw[64 * r : 64 * r + 64, cols].astype(F32)
            sums = sums + jnp.sum((w * w).reshape(8, 8, LANES), axis=0)
        scale = lax.rsqrt(jnp.sum(sums, axis=0, keepdims=True) + EPSILON)
        out[:, cols] = jnp.broadcast_to(scale, (8, LANES))
        return carry

    lax.fori_loop(0, COLS // LANES, chunk, 0, unroll=4)


def lane_sums(ref, groups):
    sums = [
        jnp.sum(ref[q * LANES : (q + 1) * LANES, :].T, axis=0, keepdims=True) for q in range(groups)
    ]
    return jnp.concatenate(sums, axis=0) if groups > 1 else sums[0]


def kernel(
    y_n, c_n, z_n,
    tf_hbm, sf_hbm, pair_hbm, weight_hbm, tp_hbm, sp_hbm,
    grad_ref, loss_ref,
    tf, sf, pair, weight, tp, sp, t_scale, s_scale, t, e, tu, su, part, spart, ubuf, v, csum, acc,
    r1p, r1z, r2p, r2z, tot_p, tot_sum, tot_z, pairs,
    a_out, a_mid, a_pre, a_in, az_out, az_in, a_all, col_sums,
    ct_out, ct_in, cz_out, cz_in, pick_out, pick_in, r3p, r3z,
    load, tu_r, th_r,
    tu_s, th_s, su_s, su_r, sh_s, sh_r, pr_s, pr_r, r1p_s, r1p_r, r1z_s, r1z_r,
    r2p_s, r2p_r, r2z_s, r2z_r, tp_s, tp_r, tz_s, tz_r, a_s, a_r, az_s, az_r, ag_s, ag_r,
    am_s, am_r, cs_s, cs_r, ct_s, ct_r, cz_s, cz_r, ca_s, ca_r, r3p_s, r3p_r, r3z_s, r3z_r,
):
    my_y, my_c, my_z = (lax.axis_index(a) for a in ("image", "crop", "proto"))
    side = lax.rem(my_c, 2)
    partner = my_c + 1 - 2 * side

    loads = [
        pltpu.make_async_copy(src, dst, load.at[k])
        for k, (src, dst) in enumerate(
            ((tf_hbm, tf), (sf_hbm, sf), (tp_hbm, tp), (sp_hbm, sp), (pair_hbm, pair), (weight_hbm, weight))
        )
    ]

    def far_first(k):
        step = k + 1
        return z_n // 2 + (1 - 2 * lax.rem(step, 2)) * (step // 2)

    def push(src, dst, sends, recvs, axis, peer):
        pltpu.make_async_remote_copy(
            src_ref=src, dst_ref=dst, send_sem=sends, recv_sem=recvs,
            device_id={axis: peer}, device_id_type=MESH,
        ).start()

    def to_crops(src, dst, sends, recvs):
        def one(k):
            peer = lax.rem(my_c + lax.rem(k + 2, c_n - 1) + 1, c_n)
            push(src(peer), dst, sends, recvs, "crop", peer)

        every(c_n - 1, one)

    def to_protos(src, dst, sends, recvs):
        def one(k):
            peer = lax.rem(my_z + far_first(k), z_n)
            push(src(peer), dst, sends, recvs, "proto", peer)

        every(z_n - 1, one)

    def await_bytes(ref, n, sem):
        some = ref.at[pl.ds(0, n)]
        pltpu.make_async_copy(some, some, sem).wait()

    barrier = pltpu.get_barrier_semaphore()

    def greet(peer):
        pl.semaphore_signal(barrier, inc=1, device_id=peer, device_id_type=MESH)

    def plane_peer(k):
        step = lax.rem(k + 15, y_n * c_n - 1) + 1
        return {
            "image": lax.rem(my_y + step // c_n, y_n),
            "crop": lax.rem(my_c + lax.rem(step, c_n), c_n),
        }

    every(z_n - 1, lambda k: greet({"proto": lax.rem(my_z + far_first(k), z_n)}))
    for copy in loads:
        copy.start()
    every(y_n * c_n - 1, lambda k: greet(plane_peer(k)))

    loads[0].wait()
    for g in range(2):
        tu[my_y, g] = unit_rows(tf[:, g, :].astype(F32)).astype(BF16)
    loads[1].wait()
    su[my_c] = unit_rows(sf[...].astype(F32)).astype(BF16)
    loads[4].wait()
    pairs[my_c] = pair[...].astype(F32)
    loads[2].wait()
    column_scales(tp, t_scale)

    def transport(y, own):
        def chunk(i):
            for k in range(4):
                cols = pl.ds(pl.multiple_of((i * 4 + k) * CHUNK, CHUNK), CHUNK)
                rows = tu[y].reshape(LANES, ROWS)
                product = jnp.dot(rows, tp[:, cols], preferred_element_type=F32)
                terms = jnp.exp2(product * (t_scale[0:1, cols] * TEACHER))
                t[pl.ds(pl.multiple_of(y * LANES, LANES), LANES), cols] = terms
                if own:
                    csum[:, cols] = jnp.sum(terms.reshape(LANES // 8, 8, CHUNK), axis=0)

        every(2, chunk)

    transport(my_y, True)
    for k in range(COLS // LANES):
        cols = slice(k * LANES, (k + 1) * LANES)
        col_sums[my_y, :, cols] = jnp.sum(csum[:, cols], axis=0, keepdims=True)
    loads[3].wait()
    column_scales(sp, s_scale)

    pl.semaphore_wait(barrier, y_n * c_n + z_n - 2)

    def give_sums(k):
        peer = lax.rem(my_y + 2 - k + 3 * (k // 2), y_n)
        push(col_sums.at[my_y], col_sums.at[my_y], cs_s, cs_r, "image", peer)

    every(y_n - 1, give_sums)

    def give_rows(k):
        peer = lax.rem(my_y + 2 * k + 1 - 3 * (k // 2), y_n)
        push(tu.at[my_y, side], tu.at[my_y, side], tu_s, tu_r.at[my_y], "image", peer)

    every(y_n - 1, give_rows)

    def give_students(k):
        peer = lax.rem(my_c + 2 * k + 2, c_n)
        push(su.at[my_c], su.at[my_c], su_s, su_r, "crop", peer)

    every(c_n // 2 - 1, give_students)
    push(su.at[my_c], su.at[my_c], sh_s, sh_r, "crop", partner)
    to_crops(lambda peer: pairs.at[my_c], pairs.at[my_c], pr_s, pr_r)

    def hand_over(y):
        pltpu.make_async_copy(tu.at[y, side], tu.at[y, side], tu_r.at[y]).wait()
        push(tu.at[y, side], tu.at[y, side], th_s, th_r.at[y], "crop", partner)

    def handed(y):
        pltpu.make_async_copy(tu.at[y, side], tu.at[y, side], th_r.at[y]).wait()

    def set_v(sums):
        for k, s in enumerate(sums):
            v[:, k * LANES : (k + 1) * LANES] = jnp.broadcast_to(
                1.0 / jnp.sum(s, axis=0, keepdims=True), (8, LANES)
            )

    def row_pass(first, n):
        def block(r, carry):
            rows = pl.ds(pl.multiple_of(first + r * 8, 8), 8)
            total = t[rows, 0:LANES] * v[:, 0:LANES]
            for k in range(1, COLS // LANES):
                cols = slice(k * LANES, (k + 1) * LANES)
                total = total + t[rows, cols] * v[:, cols]
            part[pl.ds(pl.multiple_of(r * 8, 8), 8), :] = total
            return carry

        lax.fori_loop(0, n // 8, block, 0, unroll=4)
        return lane_sums(part, n // LANES)

    def column_pass(row_sums):
        u = 1.0 / row_sums
        for q in range(ROWS // LANES):
            ubuf[q * LANES : (q + 1) * LANES, :] = jnp.broadcast_to(u[q : q + 1, :], (LANES, LANES)).T

        def block(r, sums):
            rows = pl.ds(pl.multiple_of(r * 8, 8), 8)
            scale = ubuf[rows, :]
            return tuple(
                s + t[rows, k * LANES : (k + 1) * LANES] * scale for k, s in enumerate(sums)
            )

        zero = tuple(jnp.zeros((8, LANES), F32) for _ in range(COLS // LANES))
        set_v(lax.fori_loop(0, ROWS // 8, block, zero, unroll=4))

    await_bytes(col_sums, y_n - 1, cs_r)
    v[...] = jnp.broadcast_to(1.0 / jnp.sum(col_sums[...], axis=0), (8, COLS))
    mine_1 = my_y * c_n + my_c
    r1p[mine_1] = row_pass(my_y * LANES, LANES)

    def give_first(k):
        pltpu.make_async_remote_copy(
            src_ref=r1p.at[mine_1], dst_ref=r1p.at[mine_1], send_sem=r1p_s, recv_sem=r1p_r,
            device_id=plane_peer(k), device_id_type=MESH,
        ).start()

    every(y_n * c_n - 1, give_first)

    others = [lax.rem(my_y + k, y_n) for k in (1, 3, 2)]
    hand_over(others[0])
    hand_over(others[1])
    handed(others[0])
    transport(others[0], False)
    hand_over(others[2])
    await_bytes(su, c_n // 2 - 1, su_r)

    def hand_students(k):
        slot = lax.rem(my_c + 2 * k + 2, c_n)
        push(su.at[slot], su.at[slot], sh_s, sh_r, "crop", partner)

    every(c_n // 2 - 1, hand_students)
    handed(others[1])
    transport(others[1], False)
    handed(others[2])
    transport(others[2], False)

    await_bytes(r1p, y_n * c_n - 1, r1p_r)
    firsts = [jnp.sum(r1p[c_n * y : c_n * y + c_n], axis=0) for y in range(y_n)]
    r1z[my_z] = jnp.concatenate(firsts, axis=0).astype(BF16)
    to_protos(lambda peer: r1z.at[my_z], r1z.at[my_z], r1z_s, r1z_r)

    await_bytes(su, c_n // 2, sh_r)
    spart[...] = jnp.zeros_like(spart)

    def student(i):
        for k in range(2):
            cols = pl.ds(pl.multiple_of((2 * i + k) * CHUNK, CHUNK), CHUNK)
            for h in range(2):
                some = slice(256 * h, 256 * h + 256)
                rows = su[4 * h : 4 * h + 4].reshape(256, ROWS)
                product = jnp.dot(rows, sp[:, cols], preferred_element_type=F32)
                scale = s_scale[0:1, cols]
                terms = jnp.exp2(product * (scale * STUDENT))
                spart[some, :] += terms[:, :LANES] + terms[:, LANES:]
                e[some, cols] = (terms * scale).astype(BF16)

    every(COLS // CHUNK // 2, student)

    for j in range(2):
        some = slice(j * CHUNK, (j + 1) * CHUNK)
        acc[:, some] = lax.dot_general(e[...], sp[some, :], NT, preferred_element_type=F32)
    for c in range(c_n):
        rows = slice(64 * c, 64 * c + 64)
        unit = su[c].astype(F32)
        product = acc[rows, :] * unit
        shares = product[:, :LANES]
        for k in range(1, 4):
            shares = shares + product[:, k * LANES : (k + 1) * LANES]
        part[rows, :] = shares
        alpha = jnp.sum(shares, axis=1, keepdims=True)
        a_out[c % 2, c // 2] = (acc[rows, :] - alpha * unit).astype(BF16)
    push(a_out.at[1 - side], a_mid, am_s, am_r, "crop", partner)
    tot_p[my_c] = jnp.concatenate([lane_sums(spart, 4), lane_sums(part, 4)], axis=0)
    to_crops(lambda peer: tot_p.at[my_c], tot_p.at[my_c], tp_s, tp_r)
    pltpu.make_async_copy(a_mid, a_mid, am_r).wait()
    my_x = my_c // 2

    def merge(x):
        a_pre[x] = (a_out[side, x].astype(F32) + a_mid[x].astype(F32)).astype(BF16)

    every(c_n // 2, merge)

    def give_parts(k):
        x = lax.rem(my_x + k + 1, c_n // 2)
        push(a_pre.at[x], a_in.at[my_x], a_s, a_r, "crop", 2 * x + side)

    every(c_n // 2 - 1, give_parts)

    await_bytes(r1z, z_n - 1, r1z_r)
    column_pass(jnp.sum(r1z[...].astype(F32), axis=0))
    r2p[my_c] = row_pass(0, ROWS)
    to_crops(lambda peer: r2p.at[my_c], r2p.at[my_c], r2p_s, r2p_r)

    await_bytes(r2p, c_n - 1, r2p_r)
    r2z[my_z] = jnp.sum(r2p[...], axis=0).astype(BF16)
    to_protos(lambda peer: r2z.at[my_z], r2z.at[my_z], r2z_s, r2z_r)
    await_bytes(a_in, c_n // 2 - 1, a_r)
    a_in[my_x] = a_pre[my_x]
    for g in range(8):
        rows = slice(g * 8, g * 8 + 8)
        total = a_in[0, rows, :].astype(F32)
        for k in range(1, c_n // 2):
            total = total + a_in[k, rows, :].astype(F32)
        for h in range(2):
            az_out[2 * g + h] = total[:, h * 256 : (h + 1) * 256].astype(BF16)
    await_bytes(tot_p, c_n - 1, tp_r)
    whole = jnp.sum(tot_p[...], axis=0)
    for q in range(4):
        tot_sum[q] = jnp.concatenate([whole[q : q + 1, :], whole[q + 4 : q + 5, :]], axis=0)
    tot_z[my_z] = tot_sum[my_c // 2]

    to_protos(lambda peer: az_out.at[peer], az_in.at[my_z], az_s, az_r)
    to_protos(lambda peer: tot_z.at[my_z], tot_z.at[my_z], tz_s, tz_r)

    await_bytes(r2z, z_n - 1, r2z_r)
    column_pass(jnp.sum(r2z[...].astype(F32), axis=0))

    own_rows = pl.ds(pl.multiple_of(my_y * LANES, LANES), LANES)
    for k in range(COLS // CHUNK):
        cols = slice(k * CHUNK, (k + 1) * CHUNK)
        scaled = t[own_rows, cols] * v[0:1, cols]
        e[0:LANES, cols] = (scaled * s_scale[0:1, cols]).astype(BF16)
        halves = scaled[:, :LANES] + scaled[:, LANES:]
        part[0:LANES, :] = halves if k == 0 else part[0:LANES, :] + halves
    r3p[my_c] = lane_sums(part, 1)
    to_crops(lambda peer: r3p.at[my_c], r3p.at[my_c], r3p_s, r3p_r)
    sums = lax.dot_general(e[0:LANES, :], sp[...], NT, preferred_element_type=F32)
    for c in range(c_n):
        for g in range(2):
            ct_out[c, g] = sums[64 * g + 8 * c : 64 * g + 8 * c + 8, :].astype(BF16)
    to_crops(lambda peer: ct_out.at[peer], ct_in.at[my_c], ct_s, ct_r)
    ct_in[my_c] = ct_out[my_c]

    await_bytes(az_in, z_n - 1, az_r)
    az_in[my_z] = az_out[my_z]
    a_all[my_z] = jnp.sum(az_in[...].astype(F32), axis=0).astype(BF16)
    to_protos(lambda peer: a_all.at[my_z], a_all.at[my_z], ag_s, ag_r)

    await_bytes(r3p, c_n - 1, r3p_r)
    r3z[my_z] = jnp.sum(r3p[...], axis=0)
    to_protos(lambda peer: r3z.at[my_z], r3z.at[my_z], r3z_s, r3z_r)
    await_bytes(ct_in, c_n - 1, ct_r)
    total = jnp.sum(ct_in[...].astype(F32), axis=0)
    mine = lax.rem(my_z, 4)
    for k in range(4):
        tile = total[:, :, k * LANES : (k + 1) * LANES].reshape(16, LANES)
        cz_out[k] = tile.astype(BF16)
    to_protos(lambda peer: cz_out.at[lax.rem(peer, 4)], cz_in.at[my_z], cz_s, cz_r)
    cz_in[my_z] = cz_out[mine]

    images = ROWS // c_n
    lane = lax.broadcasted_iota(jnp.int32, (images, LANES), 1)
    row = lax.broadcasted_iota(jnp.int32, (images, LANES), 0)

    def as_column(values, first, rows):
        n = values.shape[1]
        wide = jnp.broadcast_to(values, (rows, n))
        picked = jnp.where(lane[:rows, :n] == row[:rows, :n] + first, wide, jnp.zeros_like(wide))
        return jnp.sum(picked, axis=1, keepdims=True)

    loads[5].wait()
    weights = as_column(weight[...].astype(F32), 0, images)
    x = sf[...].astype(F32)
    unit = su[my_c].astype(F32)
    norm = lax.rsqrt(jnp.sum(x * x, axis=1, keepdims=True) + EPSILON)
    await_bytes(pairs, c_n - 1, pr_r)
    views = [as_column(pairs[c], my_c * 8, 8) > 0.5 for c in range(c_n)]
    await_bytes(tot_z, z_n - 1, tz_r)
    both = jnp.sum(tot_z[...], axis=0)
    totals = as_column(both[0:1, :], side * images, images)
    alpha = as_column(both[1:2, :], side * images, images)
    await_bytes(r3z, z_n - 1, r3z_r)
    last = 1.0 / jnp.sum(r3z[...], axis=0)
    scales = [as_column(last, images * g + my_c * 8, 8) for g in range(2)]

    await_bytes(cz_in, z_n - 1, cz_r)
    tile = jnp.sum(cz_in[...].astype(F32), axis=0)
    sides = [tile[8 * g : 8 * g + 8] * scales[g] for g in range(2)]
    for c in range(c_n):
        pick_out[c] = jnp.where(views[c], sides[1], sides[0])
    slot = mine * c_n + my_c

    def give_picks(k):
        step = lax.rem(k + 15, 4 * c_n - 1) + 1
        peer_c = lax.rem(my_c + lax.rem(step, c_n), c_n)
        pltpu.make_async_remote_copy(
            src_ref=pick_out.at[peer_c], dst_ref=pick_in.at[slot], send_sem=ca_s, recv_sem=ca_r,
            device_id={"crop": peer_c, "proto": lax.rem(my_z + z_n + 1 - lax.rem(step // c_n + 1, 4), z_n)},
            device_id_type=MESH,
        ).start()

    every(4 * c_n - 1, give_picks)
    pick_in[slot] = pick_out[my_c]
    await_bytes(a_all, z_n - 1, ag_r)
    for g in range(8):
        for h in range(2):
            rows = slice(g * 8, g * 8 + 8)
            cols = slice(h * 256, (h + 1) * 256)
            whole = a_all[2 * g + h].astype(F32) + alpha[rows] * unit[rows, cols]
            grad_ref[rows, cols] = whole / totals[rows]
    await_bytes(pick_in, 4 * c_n - 1, ca_r)

    chosen = jnp.concatenate(
        [jnp.concatenate([pick_in[k * c_n + c] for k in range(4)], axis=1) for c in range(c_n)], axis=0
    )
    back = (weights * 10.0) * (grad_ref[...] - chosen)
    cross = jnp.sum(unit * chosen, axis=1, keepdims=True) * 10.0
    along = jnp.sum(x * back, axis=1, keepdims=True)
    grad_ref[...] = norm * back - norm * norm * norm * x * along
    losses = jnp.broadcast_to(jnp.log(totals) - cross, (images, images))
    eye = lane[:, :images] == row[:, :images]
    loss_ref[...] = jnp.sum(jnp.where(eye, losses, 0.0), axis=0, keepdims=True)

    for ref, n, sem in (
        (su, y_n - 1, tu_s), (su, y_n - 1, th_s), (col_sums, y_n - 1, cs_s),
        (su, c_n // 2 - 1, su_s), (su, c_n // 2, sh_s), (pairs, c_n - 1, pr_s),
        (r1p, y_n * c_n - 1, r1p_s), (r1z, z_n - 1, r1z_s),
        (r2p, c_n - 1, r2p_s), (r2z, z_n - 1, r2z_s), (tot_p, c_n - 1, tp_s),
        (tot_z, z_n - 1, tz_s), (a_in, c_n // 2 - 1, a_s),
        (az_in, z_n - 1, az_s), (a_all, z_n - 1, ag_s), (ct_in, c_n - 1, ct_s),
        (cz_in, z_n - 1, cz_s), (pick_in, 4 * c_n - 1, ca_s),
        (r3p, c_n - 1, r3p_s), (r3z, z_n - 1, r3z_s),
    ):
        await_bytes(ref, n, sem)
    pltpu.make_async_copy(a_mid, a_mid, am_s).wait()


def deliver(grad_in, loss_in, grad_ref, loss_ref):
    grad_ref[0] = grad_in[...]
    loss_ref[...] = loss_in[...]


def solution(mesh):
    y_n, c_n, z_n = (mesh.shape[a] for a in ("image", "crop", "proto"))

    def step(teacher_feats, student_feats, teacher_protos, student_protos, pairing, row_weight):
        images, views, width = teacher_feats.shape
        vmem = pl.BlockSpec(memory_space=pltpu.VMEM)
        hbm = pl.BlockSpec(memory_space=pltpu.HBM)
        dma = pltpu.SemaphoreType.DMA
        ram = pltpu.VMEM
        grad, loss = pl.pallas_call(
            functools.partial(kernel, y_n, c_n, z_n),
            out_shape=(
                jax.ShapeDtypeStruct((images, width), F32),
                jax.ShapeDtypeStruct((1, images), F32),
            ),
            in_specs=[hbm] * 6,
            out_specs=(vmem, vmem),
            scratch_shapes=[
                ram((images, views, width), BF16),
                ram((images, width), BF16),
                ram((1, images), jnp.int32),
                ram((1, images), BF16),
                ram((width, COLS), BF16),
                ram((width, COLS), BF16),
                ram((8, COLS), F32),
                ram((8, COLS), F32),
                ram((ROWS, COLS), F32),
                ram((ROWS, COLS), BF16),
                ram((y_n, views, images, width), BF16),
                ram((c_n, images, width), BF16),
                ram((ROWS, LANES), F32),
                ram((ROWS, LANES), F32),
                ram((ROWS, LANES), F32),
                ram((8, COLS), F32),
                ram((8, COLS), F32),
                ram((ROWS, ROWS), F32),
                ram((y_n * c_n, 1, LANES), F32),
                ram((z_n, 4, LANES), BF16),
                ram((c_n, 4, LANES), F32),
                ram((z_n, 4, LANES), BF16),
                ram((c_n, 8, LANES), F32),
                ram((4, 2, LANES), F32),
                ram((z_n, 2, LANES), F32),
                ram((c_n, 1, images), F32),
                ram((2, c_n // 2, images, width), BF16),
                ram((c_n // 2, images, width), BF16),
                ram((c_n // 2, images, width), BF16),
                ram((c_n // 2, images, width), BF16),
                ram((z_n, 8, 256), BF16),
                ram((z_n, 8, 256), BF16),
                ram((z_n, 8, 256), BF16),
                ram((y_n, 1, COLS), F32),
                ram((c_n, 2, 8, width), BF16),
                ram((c_n, 2, 8, width), BF16),
                ram((4, 16, LANES), BF16),
                ram((z_n, 16, LANES), BF16),
                ram((c_n, 8, LANES), F32),
                ram((4 * c_n, 8, LANES), F32),
                ram((c_n, 1, LANES), F32),
                ram((z_n, 1, LANES), F32),
                dma((6,)),
                dma((y_n,)),
                dma((y_n,)),
            ]
            + [dma(())] * 40,
            compiler_params=pltpu.CompilerParams(
                collective_id=0, has_side_effects=True, vmem_limit_bytes=32 * 1024 * 1024
            ),
        )(
            *(
                pltpu.with_memory_space_constraint(x, pltpu.HBM)
                for x in (
                    teacher_feats,
                    student_feats.reshape(images, width),
                    pairing,
                    row_weight,
                    teacher_protos,
                    student_protos,
                )
            )
        )
        return pl.pallas_call(
            deliver,
            out_shape=(
                jax.ShapeDtypeStruct((1, images, width), F32),
                jax.ShapeDtypeStruct((1, images), F32),
            ),
            in_specs=[vmem] * 2,
            out_specs=(vmem, vmem),
            compiler_params=pltpu.CompilerParams(vmem_limit_bytes=2 * 1024 * 1024),
        )(grad, loss)

    return jax.shard_map(
        step,
        mesh=mesh,
        in_specs=(
            P("image", None, None),
            P("crop", "image", None),
            P(None, ("crop", "proto")),
            P(None, ("crop", "proto")),
            P("crop", "image"),
            P("crop", "image"),
        ),
        out_specs=(P("crop", "image", None), P("crop", "image")),
        check_vma=False,
    )
```
